32 devices in a mesh: facet: 4 (over z), sub: 2 (over y), wa: 4 (over x, core).
Axes of the slice: x: 2, y: 2, z: 4, core: 2. Of those that a mesh axis runs over, the one named last changes fastest.
Arguments:
- facet_data: bfloat16 [4, 128, 2, 8192], P('facet', ('sub', 'wa')), may hold values from -6 to 6
- window: float32 [8192], replicated, may hold values from 0.1 to 1
- screen_phase: float32 [1024, 1024], P('facet'), may hold values from -0.5 to 0.5
- facet_shift: int32 [4], replicated, may hold values from 0 to 1023
- sub_offset: int32 [8], replicated, may hold values from 0 to 8191
- win_start: int32 [4, 8], replicated, may hold values from 0 to 512
- win_extent: int32 [4, 8], replicated, may hold values from 256 to 512, as said below
- owner_slot: int32 [8], replicated, may hold values from 0 to 7, each once
- layer_w: int32 [8], replicated, may hold values from -12 to 12
Outputs:
- layers: bfloat16 [8, 8, 1024, 2, 1024], P('sub', 'wa', 'facet')
The draws below stay inside these ranges and needn't reach their ends.
Inputs may be any that keep to these rules, and one draw needn't show every extreme that they name: win_start[f, j] + win_extent[f, j] <= 1024 for every facet f and subgrid j. A permutation of the subgrids; the subgrid with owner_slot = p belongs to sub index p // 4.
All inputs are finite; a program needn't handle non-finite values.
Results may differ from the reference program's by a relative error of at most 0.008.
Values may be sent and summed in bfloat16 or wider, within the bound.
A program may use at most 128 MiB of HBM per device.

```python
import math
import jax
import jax.numpy as jnp
from jax import lax

FN = 8192
SG = 1024
NFAC = 4
SUBS = 8
LAYERS = 8
STRIP = 128
EMAX = 512
EMIN = 256


def draw_win_extent(key, part):
    base_key = jax.random.fold_in(key, 11)
    first_key, second_key, third_key = jax.random.split(base_key, 3)
    values = jax.random.randint(first_key, (NFAC, SUBS), EMIN, EMAX + 1)
    chosen = jax.random.randint(second_key, (NFAC,), 0, SUBS)
    column = jax.random.randint(third_key, (), 0, SUBS)
    indices = jnp.arange(SUBS)
    widest = (indices[None, :] == chosen[:, None]) | (indices[None, :] == column)
    return jnp.where(widest, EMAX, values).astype(jnp.int32)


def place_ends(result, key, smallest, largest):
    dims = result.shape
    place = [jax.random.randint(jax.random.fold_in(key, axis), (), 0, dims[axis]) for axis in range(len(dims))]
    result = result.at[tuple(place)].set(smallest)
    longest = dims.index(max(dims))
    place[longest] = (place[longest] + 1) % dims[longest]
    return result.at[tuple(place)].set(largest)


def levels(rng, extent, cuts, low, high):
    def one(dim, parts):
        steps = jax.random.uniform(jax.random.fold_in(jax.random.fold_in(rng, 6), dim), (parts,), jnp.float32, low / len(cuts), high / len(cuts))
        return jnp.repeat(jnp.exp(steps), extent[dim] // parts).reshape((-1,) + (1,) * (len(extent) - dim - 1))

    gain = one(*cuts[0])
    for cut in cuts[1:]:
        gain = gain * one(*cut)
    return gain


def noise(stream_key, extent, scale, most, shards=(), kind=jnp.bfloat16):
    values = scale * jax.random.normal(stream_key, extent, jnp.float32)
    if shards:
        values = values * levels(stream_key, extent, shards, -0.22, 0.18)
    return jnp.clip(values, -most, most).astype(kind)


def setup_inputs(seed: int = 0) -> dict:
    key_list = jax.random.split(jax.random.key(seed), 10)
    return {
        "facet_data": noise(key_list[0], (NFAC, STRIP, 2, FN), 1.0, 6.0, ((0, 4), (1, 8))),
        "window": jnp.clip(jnp.exp(jax.random.uniform(key_list[1], (FN,), jnp.float32, math.log(0.1), math.log(1.0))), 0.1, 1.0),
        "screen_phase": jnp.clip(jax.random.uniform(key_list[2], (SG, SG), jnp.float32, -0.5, 0.5) * levels(key_list[2], (SG, SG), ((0, 4),), -0.4, 0.0), -0.5, 0.5),
        "facet_shift": place_ends(jax.random.randint(key_list[3], (NFAC,), 0, SG), jax.random.fold_in(key_list[3], 1), 0, SG - 1).astype(jnp.int32),
        "sub_offset": place_ends(jax.random.randint(key_list[4], (SUBS,), 0, FN), jax.random.fold_in(key_list[4], 1), 0, FN - 1).astype(jnp.int32),
        "win_start": place_ends(jax.random.randint(key_list[5], (NFAC, SUBS), 0, SG - EMAX + 1), jax.random.fold_in(key_list[5], 1), 0, SG - EMAX).astype(jnp.int32),
        "win_extent": draw_win_extent(jax.random.fold_in(key_list[9], 71), 0),
        "owner_slot": jax.random.permutation(key_list[7], SUBS).astype(jnp.int32),
        "layer_w": place_ends(jax.random.randint(key_list[8], (LAYERS,), -12, 13), jax.random.fold_in(key_list[8], 1), -12, 12).astype(jnp.int32),
    }


def phase_of(products, modulus, sign_value):
    angles = sign_value * 2.0 * math.pi / modulus * (products % modulus).astype(jnp.float32)
    return (jnp.cos(angles), jnp.sin(angles))

def phase_pair(row_ids, col_ids, modulus, sign_value):
    return phase_of(row_ids[:, None] * col_ids[None, :], modulus, sign_value)

def held_bf16(values):
    return lax.optimization_barrier(values.astype(jnp.bfloat16)).astype(jnp.float32)

def precise_dot(left, right):
    return jnp.dot(left, right, precision=lax.Precision.HIGHEST)

def reference(facet_data, window, screen_phase, facet_shift, sub_offset, win_start, win_extent, owner_slot, layer_w):
    signal = facet_data.astype(jnp.float32) * window
    spectrum = jnp.fft.fft(signal[:, :, 0] + 1j * signal[:, :, 1], axis=-1) / math.sqrt(FN)
    columns = jnp.arange(SG, dtype=jnp.int32)
    shift_cos, shift_sin = phase_pair(facet_shift, columns, SG, 1.0)
    strip_ids = jnp.arange(STRIP, dtype=jnp.int32)
    row_cos, row_sin = phase_pair(columns, strip_ids, SG, -1.0)
    row_cos = held_bf16(row_cos)
    row_sin = held_bf16(row_sin)
    fwd_cos, fwd_sin = phase_pair(columns, columns, SG, -1.0)
    fwd_cos = held_bf16(fwd_cos)
    fwd_sin = held_bf16(fwd_sin)

    def one_subgrid(sub_index):
        picked = jnp.take(spectrum, (sub_offset[sub_index] + columns) % FN, axis=2)
        begin_col = win_start[:, sub_index][:, None]
        end_col = begin_col + win_extent[:, sub_index][:, None]
        inside = (columns[None, :] >= begin_col) & (columns[None, :] < end_col)
        part_real = picked.real * shift_cos[:, None, :] - picked.imag * shift_sin[:, None, :]
        part_imag = picked.real * shift_sin[:, None, :] + picked.imag * shift_cos[:, None, :]
        part_real = held_bf16(jnp.where(inside[:, None, :], part_real, 0.0))
        part_imag = held_bf16(jnp.where(inside[:, None, :], part_imag, 0.0))
        summed = (lax.optimization_barrier(jnp.sum(part_real, 0)) + 1j * lax.optimization_barrier(jnp.sum(part_imag, 0))) / math.sqrt(NFAC)
        col_image = jnp.fft.ifft(summed, axis=-1) * math.sqrt(SG)
        q_real = held_bf16(col_image.real)
        q_imag = held_bf16(col_image.imag)
        p_real = (precise_dot(row_cos, q_real) - precise_dot(row_sin, q_imag)) / math.sqrt(STRIP)
        p_imag = (precise_dot(row_sin, q_real) + precise_dot(row_cos, q_imag)) / math.sqrt(STRIP)
        p_real = held_bf16(p_real)
        p_imag = held_bf16(p_imag)

        def one_layer(layer_value):
            turn_angles = layer_value.astype(jnp.float32) * screen_phase
            turn_cos = jnp.cos(turn_angles)
            turn_sin = jnp.sin(turn_angles)
            s_real = held_bf16(p_real * turn_cos - p_imag * turn_sin)
            s_imag = held_bf16(p_real * turn_sin + p_imag * turn_cos)
            o_real = precise_dot(s_real, fwd_cos) - precise_dot(s_imag, fwd_sin)
            o_imag = precise_dot(s_real, fwd_sin) + precise_dot(s_imag, fwd_cos)
            return (jnp.stack([o_real, o_imag], 1) / math.sqrt(SG)).astype(jnp.bfloat16)
        return lax.map(one_layer, layer_w)
    per_subgrid = lax.map(one_subgrid, jnp.arange(SUBS, dtype=jnp.int32))
    return jnp.zeros_like(per_subgrid).at[owner_slot].set(per_subgrid)
```

```python
import functools
import math

import jax
import jax.numpy as jnp
import numpy as np
from jax import lax
from jax.experimental import pallas as pl
from jax.experimental.pallas import tpu as pltpu
from jax.sharding import PartitionSpec as P

RADIX = 4
LANES = 128
PARTS = 2
MESH = pl.DeviceIdType.MESH


def table(products, modulus, sign_value):
    angles = (sign_value * 2.0 * math.pi / modulus) * (products % modulus).astype(np.float64)
    return np.cos(angles), np.sin(angles)


def sincos(angles):
    turns = jnp.floor(angles * (2.0 / math.pi) + 0.5)
    rest = angles - turns * 1.5703125
    rest = rest - turns * 4.837512969970703e-4
    rest = rest - turns * 7.549789948768648e-8
    square = rest * rest
    sine = rest + rest * square * (
        -1.6666654611e-1 + square * (8.3321608736e-3 + square * -1.9515295891e-4)
    )
    cosine = (1.0 - 0.5 * square) + square * square * (
        4.166664568298827e-2 + square * (-1.388731625493765e-3 + square * 2.443315711809948e-5)
    )
    quadrant = turns.astype(jnp.int32)
    odd = (quadrant & 1) == 1
    sin_size = jnp.where(odd, cosine, sine)
    cos_size = jnp.where(odd, sine, cosine)
    sin_value = jnp.where((quadrant & 2) == 2, -sin_size, sin_size)
    cos_value = jnp.where(((quadrant + 1) & 2) == 2, -cos_size, cos_size)
    return cos_value, sin_value


def strip_tables(facet_len, grid_size):
    inner_len = LANES
    outer_len = facet_len // inner_len
    outer_ids = np.arange(outer_len)
    inner_ids = np.arange(inner_len)
    c1, s1 = table(outer_ids[:, None] * outer_ids[None, :], outer_len, -1.0)
    first = np.block([[c1, -s1], [s1, c1]]).astype(jnp.bfloat16)
    ct, st = table(outer_ids[:, None] * inner_ids[None, :], facet_len, -1.0)
    twiddle = np.stack([ct, st]).astype(np.float32)
    fold = LANES // outer_len
    q_ids = (np.arange(inner_len // fold)[None, :] * fold + np.arange(fold)[:, None]).reshape(-1)
    c2, s2 = table(q_ids[:, None] * inner_ids[None, :], inner_len, -1.0)
    scale = 1.0 / math.sqrt(facet_len)
    second = (np.block([[c2, -s2], [s2, c2]]) * scale).astype(jnp.bfloat16)
    part = grid_size // RADIX
    v_ids = np.arange(part)[None, :] * RADIX + np.arange(RADIX)[:, None]
    bc, bs = table(np.arange(part)[None, :, None] * v_ids[:, None, :], grid_size, 1.0)
    back = np.concatenate([bc, bs], 2).astype(jnp.bfloat16)
    return first, twiddle, second, back


def column_kernel(
    dims,
    shift_ref,
    offset_ref,
    start_ref,
    extent_ref,
    slot_ref,
    level_ref,
    sig_ref,
    first_ref,
    twiddle_ref,
    second_ref,
    back_ref,
    phase_ref,
    gather_ref,
    cos_ref,
    sin_ref,
    mid,
    spec,
    turn,
    outgoing,
    incoming,
    wide,
    pack_send,
    pack_recv,
    plane_send,
    block_recv,
):
    facets, owners, teams, strip_rows, facet_len, grid_size, slots, total_subs = dims
    facet_id = lax.axis_index("facet")
    sub_id = lax.axis_index("sub")
    team_id = lax.axis_index("wa")
    group = facets // slots
    chunk = strip_rows // group
    width = grid_size // 2
    part = grid_size // RADIX
    cores = 2
    spread = teams // cores
    core_id = lax.rem(team_id, cores)
    sibling = team_id + 1 - 2 * core_id

    def team_at(step):
        return lax.rem(team_id + cores * step, teams)

    barrier = pltpu.get_barrier_semaphore()
    peers = 0
    for off in range(facets):
        for turn_o in range(owners):
            if off or turn_o:
                pl.semaphore_signal(
                    barrier,
                    inc=1,
                    device_id=(lax.rem(facet_id + off, facets), lax.rem(sub_id + turn_o, owners), team_id),
                    device_id_type=MESH,
                )
                peers += 1
    for step in range(1, spread):
        pl.semaphore_signal(
            barrier, inc=1, device_id=(facet_id, sub_id, team_at(step)), device_id_type=MESH
        )
        peers += 1
    pl.semaphore_signal(barrier, inc=1, device_id=(facet_id, sub_id, sibling), device_id_type=MESH)
    peers += 1

    def holder(slot):
        def look(j, found):
            return jnp.where(slot_ref[j] == slot, j, found)

        return lax.fori_loop(0, total_subs, look, jnp.int32(0))

    outer_len = facet_len // LANES
    fold = LANES // outer_len
    tw_cos = twiddle_ref[0]
    tw_sin = twiddle_ref[1]

    def first_step(r, carry):
        got = jnp.dot(first_ref[...], sig_ref[r], preferred_element_type=jnp.float32)
        real, imag = got[:outer_len], got[outer_len:]
        rows = pl.ds(pl.multiple_of(r * outer_len, outer_len), outer_len)
        mid[rows, :LANES] = (real * tw_cos - imag * tw_sin).astype(jnp.bfloat16)
        mid[rows, LANES:] = (real * tw_sin + imag * tw_cos).astype(jnp.bfloat16)
        return carry

    lax.fori_loop(0, strip_rows, first_step, 0)
    tall = LANES // fold
    lane = lax.broadcasted_iota(jnp.int32, (tall, LANES), 1)

    def second_step(i, carry):
        rows = pl.ds(pl.multiple_of(i * LANES, LANES), LANES)
        got = lax.dot_general(
            second_ref[...], mid[rows, :], (((1,), (1,)), ((), ())), preferred_element_type=jnp.float32
        )
        for c in range(2):
            even = got[c * LANES : c * LANES + tall]
            odd = got[c * LANES + tall : (c + 1) * LANES]
            near = jnp.where(lane < outer_len, even, pltpu.roll(odd, outer_len, 1))
            far = jnp.where(lane < outer_len, pltpu.roll(even, outer_len, 1), odd)
            spec[c * tall : (c + 1) * tall, i * fold, :] = near
            spec[c * tall : (c + 1) * tall, i * fold + 1, :] = far
        return carry

    lax.fori_loop(0, strip_rows // fold, second_step, 0)

    held = [holder(p) for p in range(total_subs)]
    row_ids = lax.broadcasted_iota(jnp.int32, (total_subs, width), 0)
    k_ids = lax.broadcasted_iota(jnp.int32, (total_subs, width), 1)
    starts = jnp.zeros((total_subs, width), jnp.int32)
    extents = jnp.zeros((total_subs, width), jnp.int32)
    for p in range(total_subs):
        starts = jnp.where(row_ids == p, start_ref[facet_id, held[p]], starts)
        extents = jnp.where(row_ids == p, extent_ref[facet_id, held[p]], extents)
    product = (shift_ref[facet_id] * (starts + k_ids)) & (grid_size - 1)
    turn_cos, turn_sin = sincos(product.astype(jnp.float32) * (2.0 * math.pi / grid_size))
    inside = k_ids < extents
    turn_cos = jnp.where(inside, turn_cos, 0.0)
    turn_sin = jnp.where(inside, turn_sin, 0.0)
    for p in range(total_subs):
        turn[0, p] = turn_cos[p : p + 1]
        turn[1, p] = turn_sin[p : p + 1]

    pl.semaphore_wait(barrier, peers)

    wide_lane = lax.broadcasted_iota(jnp.int32, (strip_rows, LANES), 1)
    pieces = width // LANES
    my_slot = facet_id // group
    packs = []
    order = [s for s in range(slots // 2, slots)] + [s for s in range(slots // 2)][::-1]
    for step in order:
        for turn_o in list(range(1, owners)) + [0]:
            slot = lax.rem(my_slot + step, slots)
            owner = lax.rem(sub_id + turn_o, owners)
            p = owner * slots + slot
            j = holder(p)
            begin = lax.rem(offset_ref[j] + start_ref[facet_id, j], facet_len)
            q0 = lax.div(begin, LANES)
            shift = begin - q0 * LANES
            back_by = lax.rem(LANES - shift, LANES)
            tiles = []
            for c in range(2):
                rolled = []
                for q in range(pieces + 1):
                    tile = spec[c * tall + lax.rem(q0 + q, tall)]
                    rolled.append(pltpu.roll(tile, back_by, 1))
                tiles.append(
                    [jnp.where(wide_lane < LANES - shift, rolled[q], rolled[q + 1]) for q in range(pieces)]
                )
            reals, imags = [], []
            for q in range(pieces):
                lanes = slice(q * LANES, (q + 1) * LANES)
                cos = turn[0, p, :, lanes]
                sin = turn[1, p, :, lanes]
                reals.append(tiles[0][q] * cos - tiles[1][q] * sin)
                imags.append(tiles[0][q] * sin + tiles[1][q] * cos)
            block = jnp.concatenate(reals + imags, 1).astype(jnp.bfloat16)
            for g in range(group):
                target = slot * group + g
                piece = block[g * chunk : (g + 1) * chunk]
                n = len(packs)
                outgoing[n] = piece
                here = group == 1 and step == 0 and turn_o == 0
                if here:
                    incoming[facet_id, sub_id] = piece
                    packs.append((None, None))
                    continue
                copy = pltpu.make_async_remote_copy(
                    src_ref=outgoing.at[n],
                    dst_ref=incoming.at[facet_id, sub_id],
                    send_sem=pack_send.at[n],
                    recv_sem=pack_recv.at[facet_id, sub_id],
                    device_id=(target, owner, team_id),
                    device_id_type=MESH,
                )
                if step == 0 and turn_o == 0:
                    away = target != facet_id
                    pl.when(away)(copy.start)

                    @pl.when(target == facet_id)
                    def _():
                        incoming[facet_id, sub_id] = piece

                    packs.append((copy, away))
                else:
                    copy.start()
                    packs.append((copy, True))

    for p in range(RADIX):
        wide[p, :part] = back_ref[p]
        wide[p, part:, :part] = -back_ref[p][:, part:]
        wide[p, part:, part:] = back_ref[p][:, :part]
    mine = holder(sub_id * slots + my_slot)
    f_rows = lax.broadcasted_iota(jnp.int32, (facets, grid_size), 0)
    at = lax.broadcasted_iota(jnp.int32, (facets, grid_size), 1)
    v_ids = (at % part) * RADIX + at // part
    begins = jnp.zeros((facets, grid_size), jnp.int32)
    for f in range(facets):
        begins = jnp.where(f_rows == f, start_ref[f, mine], begins)
    ramp_cos, ramp_sin = sincos(
        ((begins * v_ids) & (grid_size - 1)).astype(jnp.float32) * (2.0 * math.pi / grid_size)
    )
    scale_col = 1.0 / math.sqrt(facets * grid_size)
    ramp_cos = ramp_cos * scale_col
    ramp_sin = ramp_sin * scale_col

    band = phase_ref.shape[0]
    block_v = LANES * RADIX
    from_ids = lax.broadcasted_iota(jnp.int32, (block_v, block_v), 0)
    to_ids = lax.broadcasted_iota(jnp.int32, (block_v, block_v), 1)
    chosen = (from_ids == (to_ids % LANES) * RADIX + to_ids // LANES).astype(jnp.float32).astype(jnp.bfloat16)
    for h in range(grid_size // block_v):
        whole = phase_ref[:, h * block_v : (h + 1) * block_v]
        ordered = jnp.zeros((band, block_v), jnp.float32)
        for level in range(3):
            digit = whole.astype(jnp.bfloat16)
            whole = whole - digit.astype(jnp.float32)
            ordered = ordered + jnp.dot(digit, chosen, preferred_element_type=jnp.float32)
        for p in range(RADIX):
            lanes = slice(p * part + h * LANES, p * part + (h + 1) * LANES)
            for l in range(cos_ref.shape[0]):
                level_value = level_ref[team_id * cos_ref.shape[0] + l].astype(jnp.float32)
                cos, sin = sincos(level_value * ordered[:, p * LANES : (p + 1) * LANES])
                cos_ref[l, :, lanes] = cos
                sin_ref[l, :, lanes] = sin

    for off in range(facets):
        for turn_o in range(owners):
            if off or turn_o:
                f = lax.rem(facet_id + off, facets)
                o = lax.rem(sub_id + turn_o, owners)
                pltpu.make_async_remote_copy(
                    src_ref=incoming.at[f, o],
                    dst_ref=incoming.at[f, o],
                    send_sem=pack_send.at[0],
                    recv_sem=pack_recv.at[f, o],
                    device_id=(f, o, team_id),
                    device_id_type=MESH,
                ).wait_recv()

    got = incoming[...].reshape(facets * owners * chunk, 2 * width).astype(jnp.float32)
    low_r, high_r = got[:, :part], got[:, part:width]
    low_i, high_i = got[:, width : width + part], got[:, width + part :]
    rows_f = owners * chunk
    images = [[], []]
    for p in range(RADIX):
        real, imag = [
            (low_r + high_r, low_i + high_i),
            (low_r - high_i, low_i + high_r),
            (low_r - high_r, low_i - high_i),
            (low_r + high_i, low_i - high_r),
        ][p]
        pair = jnp.concatenate([real.astype(jnp.bfloat16), imag.astype(jnp.bfloat16)], 1)
        moved = jnp.dot(pair, wide[p], preferred_element_type=jnp.float32)
        total_r = jnp.zeros((rows_f, part), jnp.float32)
        total_i = jnp.zeros((rows_f, part), jnp.float32)
        for f in range(facets):
            cos = ramp_cos[f : f + 1, p * part : (p + 1) * part]
            sin = ramp_sin[f : f + 1, p * part : (p + 1) * part]
            real = moved[f * rows_f : (f + 1) * rows_f, :part]
            imag = moved[f * rows_f : (f + 1) * rows_f, part:]
            total_r = total_r + (real * cos - imag * sin)
            total_i = total_i + (real * sin + imag * cos)
        images[0].append(total_r)
        images[1].append(total_i)
    for c in range(2):
        gather_ref[facet_id, team_id, c] = jnp.concatenate(images[c], 1).astype(jnp.bfloat16)

    def send(kind, f, team, h, target):
        return pltpu.make_async_remote_copy(
            src_ref=gather_ref.at[f, team, h],
            dst_ref=gather_ref.at[f, team, h],
            send_sem=plane_send.at[kind, f, team // cores, h],
            recv_sem=block_recv.at[f, team, h],
            device_id=target,
            device_id_type=MESH,
        )

    def arrive(f, team, h):
        send(0, f, team, h, (facet_id, sub_id, team_id)).wait_recv()

    has_next = facet_id < facets - 1
    has_last = facet_id > 0
    below = jnp.maximum(facet_id - 1, 0)
    above = jnp.minimum(facet_id + 1, facets - 1)

    def along(f, h, up, act):
        if up is None or up:

            @pl.when(has_next)
            def _():
                act(send(0, f, team_id, h, (above, sub_id, team_id)))

        if up is None or not up:

            @pl.when(has_last)
            def _():
                act(send(0 if up is not None else 1, f, team_id, h, (below, sub_id, team_id)))

        for step in range(1, spread):
            act(send(1 + step, f, team_id, h, (facet_id, sub_id, team_at(step))))
        act(send(1 + spread, f, team_id, h, (facet_id, sub_id, sibling)))

    def aside(f, team, h, act):
        act(send(1 + spread, f, team, h, (facet_id, sub_id, sibling)))

    def start(copy):
        copy.start()

    def finish_send(copy):
        copy.wait_send()

    def guarded(condition, body):
        if condition is None:
            body()
        else:
            pl.when(condition)(body)

    def sides(d):
        yield True, facet_id >= d, jnp.maximum(facet_id - d, 0)
        yield False, facet_id < facets - d, jnp.minimum(facet_id + d, facets - 1)

    def partners(d, h):
        for step in range(1, spread):
            if d == 0:
                arrive(facet_id, team_at(step), h)
                aside(facet_id, team_at(step), h, start)
            else:
                for _, condition, f in sides(d):

                    def body(f=f, step=step):
                        arrive(f, team_at(step), h)
                        aside(f, team_at(step), h, start)

                    pl.when(condition)(body)

    for h in range(PARTS):
        along(facet_id, h, None, start)
    for d in range(1, facets):
        for h in range(PARTS):
            for up, condition, f in sides(d):

                def body(f=f, h=h, up=up):
                    arrive(f, team_id, h)
                    along(f, h, up, start)

                pl.when(condition)(body)
            partners(d - 1, h)
    for h in range(PARTS):
        partners(facets - 1, h)
    for off in range(facets):
        for h in range(PARTS):
            f = lax.rem(facet_id + off, facets)
            for step in range(spread):
                arrive(f, lax.rem(sibling + cores * step, teams), h)

    for h in range(PARTS):
        along(facet_id, h, None, finish_send)
        for step in range(1, spread):
            aside(facet_id, team_at(step), h, finish_send)
    for d in range(1, facets):
        for h in range(PARTS):
            for up, condition, f in sides(d):

                def body(f=f, h=h, up=up):
                    along(f, h, up, finish_send)
                    for step in range(1, spread):
                        aside(f, team_at(step), h, finish_send)

                pl.when(condition)(body)
    for copy, away in packs:
        if away is True:
            copy.wait_send()
        elif away is not None:
            pl.when(away)(copy.wait_send)


def column(scalars, sig, window_rows, tables, phase, dims, layers):
    facets, owners, teams, strip_rows, facet_len, grid_size, slots, total_subs = dims
    first, twiddle, second, back = [jnp.asarray(x) for x in tables]
    group = facets // slots
    chunk = strip_rows // group
    width = grid_size // 2
    part = grid_size // RADIX
    band = phase.shape[0]
    smem = pl.BlockSpec(memory_space=pltpu.SMEM)
    vmem = pl.BlockSpec(memory_space=pltpu.VMEM)
    blocks = (facets, teams, 2, owners * chunk, grid_size)
    spread = teams // 2
    return pl.pallas_call(
        functools.partial(column_kernel, dims),
        out_shape=[
            jax.ShapeDtypeStruct(blocks, jnp.bfloat16),
            jax.ShapeDtypeStruct((layers, band, grid_size), jnp.float32),
            jax.ShapeDtypeStruct((layers, band, grid_size), jnp.float32),
        ],
        in_specs=[smem] * 6 + [vmem] * 6,
        out_specs=[vmem] * 3,
        scratch_shapes=[
            pltpu.VMEM((strip_rows * (facet_len // LANES), 2 * LANES), jnp.bfloat16),
            pltpu.VMEM((2 * facet_len // LANES, strip_rows, LANES), jnp.float32),
            pltpu.VMEM((2, total_subs, 1, width), jnp.float32),
            pltpu.VMEM((facets * owners, chunk, 2 * width), jnp.bfloat16),
            pltpu.VMEM((facets, owners, chunk, 2 * width), jnp.bfloat16),
            pltpu.VMEM((RADIX, 2 * part, 2 * part), jnp.bfloat16),
            pltpu.SemaphoreType.DMA((facets * owners,)),
            pltpu.SemaphoreType.DMA((facets, owners)),
            pltpu.SemaphoreType.DMA((2 + spread, facets, spread, PARTS)),
            pltpu.SemaphoreType.DMA((facets, teams, PARTS)),
        ],
        compiler_params=pltpu.CompilerParams(
            collective_id=0, has_side_effects=True, vmem_limit_bytes=48 * 1024 * 1024
        ),
        cost_estimate=pl.CostEstimate(flops=2_000_000_000, bytes_accessed=20_000_000, transcendentals=0),
    )(*scalars, sig, first, twiddle, second, back, phase)


def finish_kernel(band, scale_rows, left_ref, right_ref, cos_ref, sin_ref, fwd_ref, out_ref, held, wide, near, sem):
    layer = pl.program_id(1)
    grid_size = cos_ref.shape[2]
    part = grid_size // RADIX

    @pl.when((pl.program_id(0) == 0) & (layer == 0))
    def _():
        copy = pltpu.make_async_copy(left_ref.at[lax.axis_index("facet")], near, sem)
        copy.start()
        for p in range(RADIX):
            wide[p, :part] = fwd_ref[p]
            wide[p, part:, :part] = -fwd_ref[p][:, part:]
            wide[p, part:, part:] = fwd_ref[p][:, :part]
        copy.wait()

    @pl.when(layer == 0)
    def _():
        rows = jnp.dot(near[...], right_ref[0], preferred_element_type=jnp.float32)
        held[...] = (rows * scale_rows).astype(jnp.bfloat16)

    real = held[:band, :].astype(jnp.float32)
    imag = held[band:, :].astype(jnp.float32)
    cos = cos_ref[0]
    sin = sin_ref[0]
    s_real = (real * cos - imag * sin).astype(jnp.bfloat16)
    s_imag = (real * sin + imag * cos).astype(jnp.bfloat16)
    pieces = []
    for p in range(RADIX):
        lo, hi = p * part, (p + 1) * part
        pair = jnp.concatenate([s_real[:, lo:hi], s_imag[:, lo:hi]], 1)
        got = jnp.dot(pair, wide[p], preferred_element_type=jnp.float32)
        pieces.append((got[:, :part], got[:, part:]))
    (ar, ai), (br, bi), (cr, ci), (dr, di) = pieces
    er, ei, fr, fi = ar + cr, ai + ci, ar - cr, ai - ci
    gr, gi, hr, hi_ = br + dr, bi + di, br - dr, bi - di
    reals = jnp.concatenate([er + gr, fr + hi_, er - gr, fr - hi_], 1)
    imags = jnp.concatenate([ei + gi, fi - hr, ei - gi, fi + hr], 1)
    out_ref[0, 0, :, 0, :] = reals.astype(jnp.bfloat16)
    out_ref[0, 0, :, 1, :] = imags.astype(jnp.bfloat16)


def finish(left, right, cos, sin, forward, scale_rows):
    layers, band, grid_size = cos.shape
    slots, count, _ = right.shape
    part = grid_size // RADIX
    return pl.pallas_call(
        functools.partial(finish_kernel, band, scale_rows),
        grid=(slots, layers),
        out_shape=jax.ShapeDtypeStruct((slots, layers, band, 2, grid_size), jnp.bfloat16),
        in_specs=[
            pl.BlockSpec(memory_space=pl.ANY),
            pl.BlockSpec((1, count, grid_size), lambda s, l: (s, 0, 0)),
            pl.BlockSpec((1, band, grid_size), lambda s, l: (l, 0, 0)),
            pl.BlockSpec((1, band, grid_size), lambda s, l: (l, 0, 0)),
            pl.BlockSpec(forward.shape, lambda s, l: (0, 0, 0)),
        ],
        out_specs=pl.BlockSpec((1, 1, band, 2, grid_size), lambda s, l: (s, l, 0, 0, 0)),
        scratch_shapes=[
            pltpu.VMEM((2 * band, grid_size), jnp.bfloat16),
            pltpu.VMEM((RADIX, 2 * part, 2 * part), jnp.bfloat16),
            pltpu.VMEM((2 * band, count), jnp.bfloat16),
            pltpu.SemaphoreType.DMA,
        ],
        compiler_params=pltpu.CompilerParams(vmem_limit_bytes=48 * 1024 * 1024),
        cost_estimate=pl.CostEstimate(flops=10_000_000_000, bytes_accessed=20_000_000, transcendentals=0),
    )(left, right, cos, sin, forward)


def local(
    facet_data,
    window,
    screen_phase,
    facet_shift,
    sub_offset,
    win_start,
    win_extent,
    owner_slot,
    layer_w,
):
    facets = lax.axis_size("facet")
    owners = lax.axis_size("sub")
    teams = lax.axis_size("wa")
    strip_rows = facet_data.shape[1]
    facet_len = facet_data.shape[3]
    band, grid_size = screen_phase.shape
    part = grid_size // RADIX
    total_subs = owner_slot.shape[0]
    slots = total_subs // owners
    group = facets // slots
    chunk = strip_rows // group
    strip_total = strip_rows * owners * teams
    layers = layer_w.shape[0] // teams
    dims = (facets, owners, teams, strip_rows, facet_len, grid_size, slots, total_subs)

    outer_len = facet_len // LANES
    sig = (facet_data[0].astype(jnp.float32) * window).astype(jnp.bfloat16)
    sig = sig.reshape(strip_rows, 2 * outer_len, LANES)
    tables = strip_tables(facet_len, grid_size)
    scalars = (facet_shift, sub_offset, win_start, win_extent, owner_slot, layer_w)
    right, cos, sin = column(scalars, sig, window, tables, screen_phase, dims, layers)
    right = right.reshape(slots, 2 * strip_total, grid_size)

    g_ids, t_ids, c_ids, o_ids, r_ids = np.meshgrid(
        np.arange(group), np.arange(teams), np.arange(2), np.arange(owners), np.arange(chunk), indexing="ij"
    )
    global_row = ((o_ids * teams + t_ids) * strip_rows + g_ids * chunk + r_ids).reshape(1, 1, -1)
    is_imag = c_ids.reshape(1, 1, -1)
    my_rows = np.arange(grid_size).reshape(facets, band, 1)
    all_cos, all_sin = table(my_rows * global_row, grid_size, -1.0)
    real_rows = np.where(is_imag == 1, -all_sin, all_cos)
    imag_rows = np.where(is_imag == 1, all_cos, all_sin)
    left = jnp.asarray(np.concatenate([real_rows, imag_rows], 1).astype(jnp.bfloat16))

    v_ids = np.arange(part)[None, :] * RADIX + np.arange(RADIX)[:, None]
    fwd_cos, fwd_sin = table(v_ids[:, :, None] * np.arange(part)[None, None, :], grid_size, -1.0)
    rounded = lambda x: x.astype(jnp.bfloat16).astype(np.float64)
    forward = np.concatenate([rounded(fwd_cos), rounded(fwd_sin)], 2) / math.sqrt(grid_size)
    return finish(left, right, cos, sin, jnp.asarray(forward.astype(jnp.bfloat16)), 1.0 / math.sqrt(strip_total))


def solution(mesh):
    in_specs = (
        P("facet", ("sub", "wa"), None, None),
        P(),
        P("facet", None),
        P(),
        P(),
        P(),
        P(),
        P(),
        P(),
    )
    out_specs = P("sub", "wa", "facet", None, None)
    return jax.shard_map(local, mesh=mesh, in_specs=in_specs, out_specs=out_specs, check_vma=False)
```

```python
import functools
import math

import jax
import jax.numpy as jnp
import numpy as np
from jax import lax
from jax.experimental import pallas as pl
from jax.experimental.pallas import tpu as pltpu
from jax.sharding import PartitionSpec as P

RADIX = 4
LANES = 128
PARTS = 4
HALVES = 2
VMEM_COLUMN = 32 * 1024 * 1024
VMEM_FINISH = 32 * 1024 * 1024
MESH = pl.DeviceIdType.MESH


def table(products, modulus, sign_value):
    angles = (sign_value * 2.0 * math.pi / modulus) * (products % modulus).astype(np.float64)
    return np.cos(angles), np.sin(angles)


def sincos(angles):
    turns = jnp.floor(angles * (2.0 / math.pi) + 0.5)
    rest = angles - turns * 1.5703125
    rest = rest - turns * 4.837512969970703e-4
    rest = rest - turns * 7.549789948768648e-8
    square = rest * rest
    sine = rest + rest * square * (
        -1.6666654611e-1 + square * (8.3321608736e-3 + square * -1.9515295891e-4)
    )
    cosine = (1.0 - 0.5 * square) + square * square * (
        4.166664568298827e-2 + square * (-1.388731625493765e-3 + square * 2.443315711809948e-5)
    )
    quadrant = turns.astype(jnp.int32)
    odd = (quadrant & 1) == 1
    sin_size = jnp.where(odd, cosine, sine)
    cos_size = jnp.where(odd, sine, cosine)
    sin_value = jnp.where((quadrant & 2) == 2, -sin_size, sin_size)
    cos_value = jnp.where(((quadrant + 1) & 2) == 2, -cos_size, cos_size)
    return cos_value, sin_value


def strip_tables(facet_len, grid_size):
    inner_len = LANES
    outer_len = facet_len // inner_len
    outer_ids = np.arange(outer_len)
    inner_ids = np.arange(inner_len)
    c1, s1 = table(outer_ids[:, None] * outer_ids[None, :], outer_len, -1.0)
    first = np.block([[c1, -s1], [s1, c1]]).astype(jnp.bfloat16)
    ct, st = table(outer_ids[:, None] * inner_ids[None, :], facet_len, -1.0)
    twiddle = np.stack([ct, st]).astype(np.float32)
    fold = LANES // outer_len
    q_ids = (np.arange(inner_len // fold)[None, :] * fold + np.arange(fold)[:, None]).reshape(-1)
    c2, s2 = table(q_ids[:, None] * inner_ids[None, :], inner_len, -1.0)
    scale = 1.0 / math.sqrt(facet_len)
    second = (np.block([[c2, -s2], [s2, c2]]) * scale).astype(jnp.bfloat16)
    part = grid_size // RADIX
    v_ids = np.arange(part)[None, :] * RADIX + np.arange(RADIX)[:, None]
    bc, bs = table(np.arange(part)[None, :, None] * v_ids[:, None, :], grid_size, 1.0)
    back = np.concatenate([bc, bs], 2).astype(jnp.bfloat16)
    return first, twiddle, second, back


def arrivals(facets, facet_id):
    order = []
    for z in range(facets):
        row = [z]
        for d in range(1, facets):
            row += [f for f in (z - d, z + d) if 0 <= f < facets]
        order.append(row)
    picked = []
    for k in range(facets):
        value = 0
        for z in range(facets):
            gap = facet_id - z
            here = 1 - lax.div(gap * gap + (facets * facets - 1), facets * facets)
            value = value + here * order[z][k]
        picked.append(value)
    return picked


def unit(step, right_ref, slot, near_ref, fwd_ref, cos_ref, sin_ref, held, out_ref):
    layers, band, grid_size = cos_ref.shape
    part = grid_size // RADIX
    half = band // HALVES
    layer = lax.rem(step, layers)
    which = lax.div(step, layers)
    rows = pl.ds(pl.multiple_of(which * half, half), half)

    @pl.when(layer == 0)
    def _():
        right = right_ref[slot].reshape(near_ref.shape[2], grid_size)
        for p in range(RADIX):
            lanes = slice(p * part, (p + 1) * part)
            got = jnp.dot(near_ref[which], right[:, lanes], preferred_element_type=jnp.float32)
            held[:, lanes] = got.astype(jnp.bfloat16)

    pieces = []
    for p in range(RADIX):
        lanes = slice(p * part, (p + 1) * part)
        real = held[:half, lanes].astype(jnp.float32)
        imag = held[half:, lanes].astype(jnp.float32)
        cos = cos_ref[layer, rows, lanes]
        sin = sin_ref[layer, rows, lanes]
        s_real = (real * cos - imag * sin).astype(jnp.bfloat16)
        s_imag = (real * sin + imag * cos).astype(jnp.bfloat16)
        pair = jnp.concatenate([s_real, s_imag], 1)
        got = jnp.dot(pair, fwd_ref[p], preferred_element_type=jnp.float32)
        pieces.append((got[:, :part], got[:, part:]))
    (ar, ai), (br, bi), (cr, ci), (dr, di) = pieces
    er, ei, fr, fi = ar + cr, ai + ci, ar - cr, ai - ci
    gr, gi, hr, hi_ = br + dr, bi + di, br - dr, bi - di
    reals = jnp.concatenate([er + gr, fr + hi_, er - gr, fr - hi_], 1)
    imags = jnp.concatenate([ei + gi, fi - hr, ei - gi, fi + hr], 1)
    out_ref[layer, rows, 0, :] = reals.astype(jnp.bfloat16)
    out_ref[layer, rows, 1, :] = imags.astype(jnp.bfloat16)


def column_kernel(
    dims,
    shift_ref,
    offset_ref,
    start_ref,
    extent_ref,
    slot_ref,
    level_ref,
    sig_ref,
    first_ref,
    twiddle_ref,
    second_ref,
    back_ref,
    phase_ref,
    left_ref,
    gather_ref,
    cos_ref,
    sin_ref,
    near_ref,
    fwd_ref,
    done_ref,
    mid,
    spec,
    turn,
    outgoing,
    incoming,
    wide,
    held,
    pack_send,
    pack_recv,
    plane_send,
    block_recv,
    near_sem,
):
    facets, owners, teams, strip_rows, facet_len, grid_size, slots, total_subs = dims
    facet_id = lax.axis_index("facet")
    sub_id = lax.axis_index("sub")
    team_id = lax.axis_index("wa")
    group = facets // slots
    chunk = strip_rows // group
    width = grid_size // 2
    part = grid_size // RADIX
    cores = 2
    spread = teams // cores
    core_id = lax.rem(team_id, cores)
    sibling = team_id + 1 - 2 * core_id

    def team_at(step):
        return lax.rem(team_id + cores * step, teams)

    barrier = pltpu.get_barrier_semaphore()
    peers = 0
    for off in range(facets):
        for turn_o in range(owners):
            if off or turn_o:
                pl.semaphore_signal(
                    barrier,
                    inc=1,
                    device_id=(lax.rem(facet_id + off, facets), lax.rem(sub_id + turn_o, owners), team_id),
                    device_id_type=MESH,
                )
                peers += 1
    for step in range(1, spread):
        pl.semaphore_signal(
            barrier, inc=1, device_id=(facet_id, sub_id, team_at(step)), device_id_type=MESH
        )
        peers += 1
    pl.semaphore_signal(barrier, inc=1, device_id=(facet_id, sub_id, sibling), device_id_type=MESH)
    peers += 1

    near_copy = pltpu.make_async_copy(left_ref.at[facet_id], near_ref, near_sem)
    near_copy.start()

    def holder(slot):
        def look(j, found):
            return jnp.where(slot_ref[j] == slot, j, found)

        return lax.fori_loop(0, total_subs, look, jnp.int32(0))

    outer_len = facet_len // LANES
    fold = LANES // outer_len
    tw_cos = twiddle_ref[0]
    tw_sin = twiddle_ref[1]

    def first_step(r, carry):
        got = jnp.dot(first_ref[...], sig_ref[r], preferred_element_type=jnp.float32)
        real, imag = got[:outer_len], got[outer_len:]
        rows = pl.ds(pl.multiple_of(r * outer_len, outer_len), outer_len)
        mid[rows, :LANES] = (real * tw_cos - imag * tw_sin).astype(jnp.bfloat16)
        mid[rows, LANES:] = (real * tw_sin + imag * tw_cos).astype(jnp.bfloat16)
        return carry

    lax.fori_loop(0, strip_rows, first_step, 0)
    tall = LANES // fold
    lane = lax.broadcasted_iota(jnp.int32, (tall, LANES), 1)

    def second_step(i, carry):
        rows = pl.ds(pl.multiple_of(i * LANES, LANES), LANES)
        got = lax.dot_general(
            second_ref[...], mid[rows, :], (((1,), (1,)), ((), ())), preferred_element_type=jnp.float32
        )
        for c in range(2):
            even = got[c * LANES : c * LANES + tall]
            odd = got[c * LANES + tall : (c + 1) * LANES]
            near = jnp.where(lane < outer_len, even, pltpu.roll(odd, outer_len, 1))
            far = jnp.where(lane < outer_len, pltpu.roll(even, outer_len, 1), odd)
            spec[c * tall : (c + 1) * tall, i * fold, :] = near
            spec[c * tall : (c + 1) * tall, i * fold + 1, :] = far
        return carry

    lax.fori_loop(0, strip_rows // fold, second_step, 0)

    holders = [holder(p) for p in range(total_subs)]
    row_ids = lax.broadcasted_iota(jnp.int32, (total_subs, width), 0)
    k_ids = lax.broadcasted_iota(jnp.int32, (total_subs, width), 1)
    starts = jnp.zeros((total_subs, width), jnp.int32)
    extents = jnp.zeros((total_subs, width), jnp.int32)
    for p in range(total_subs):
        starts = jnp.where(row_ids == p, start_ref[facet_id, holders[p]], starts)
        extents = jnp.where(row_ids == p, extent_ref[facet_id, holders[p]], extents)
    product = (shift_ref[facet_id] * (starts + k_ids)) & (grid_size - 1)
    turn_cos, turn_sin = sincos(product.astype(jnp.float32) * (2.0 * math.pi / grid_size))
    inside = k_ids < extents
    turn_cos = jnp.where(inside, turn_cos, 0.0)
    turn_sin = jnp.where(inside, turn_sin, 0.0)
    for p in range(total_subs):
        turn[0, p] = turn_cos[p : p + 1]
        turn[1, p] = turn_sin[p : p + 1]

    pl.semaphore_wait(barrier, peers)

    wide_lane = lax.broadcasted_iota(jnp.int32, (strip_rows, LANES), 1)
    pieces = width // LANES
    my_slot = facet_id // group
    packs = []
    order = [s for s in range(slots // 2, slots)] + [s for s in range(slots // 2)][::-1]
    for step in order:
        for turn_o in list(range(1, owners)) + [0]:
            slot = lax.rem(my_slot + step, slots)
            owner = lax.rem(sub_id + turn_o, owners)
            p = owner * slots + slot
            j = holder(p)
            begin = lax.rem(offset_ref[j] + start_ref[facet_id, j], facet_len)
            q0 = lax.div(begin, LANES)
            shift = begin - q0 * LANES
            back_by = lax.rem(LANES - shift, LANES)
            tiles = []
            for c in range(2):
                rolled = []
                for q in range(pieces + 1):
                    tile = spec[c * tall + lax.rem(q0 + q, tall)]
                    rolled.append(pltpu.roll(tile, back_by, 1))
                tiles.append(
                    [jnp.where(wide_lane < LANES - shift, rolled[q], rolled[q + 1]) for q in range(pieces)]
                )
            reals, imags = [], []
            for q in range(pieces):
                lanes = slice(q * LANES, (q + 1) * LANES)
                cos = turn[0, p, :, lanes]
                sin = turn[1, p, :, lanes]
                reals.append(tiles[0][q] * cos - tiles[1][q] * sin)
                imags.append(tiles[0][q] * sin + tiles[1][q] * cos)
            block = jnp.concatenate(reals + imags, 1).astype(jnp.bfloat16)
            for g in range(group):
                target = slot * group + g
                piece = block[g * chunk : (g + 1) * chunk]
                n = len(packs)
                outgoing[n] = piece
                here = group == 1 and step == 0 and turn_o == 0
                if here:
                    incoming[facet_id, sub_id] = piece
                    packs.append((None, None))
                    continue
                copy = pltpu.make_async_remote_copy(
                    src_ref=outgoing.at[n],
                    dst_ref=incoming.at[facet_id, sub_id],
                    send_sem=pack_send.at[n],
                    recv_sem=pack_recv.at[facet_id, sub_id],
                    device_id=(target, owner, team_id),
                    device_id_type=MESH,
                )
                if step == 0 and turn_o == 0:
                    away = target != facet_id
                    pl.when(away)(copy.start)

                    @pl.when(target == facet_id)
                    def _():
                        incoming[facet_id, sub_id] = piece

                    packs.append((copy, away))
                else:
                    copy.start()
                    packs.append((copy, True))

    for p in range(RADIX):
        wide[p, :part] = back_ref[p]
        wide[p, part:, :part] = -back_ref[p][:, part:]
        wide[p, part:, part:] = back_ref[p][:, :part]
        fwd_ref[p] = wide[p].T
    mine = holder(sub_id * slots + my_slot)
    f_rows = lax.broadcasted_iota(jnp.int32, (facets, grid_size), 0)
    at = lax.broadcasted_iota(jnp.int32, (facets, grid_size), 1)
    v_ids = (at % part) * RADIX + at // part
    begins = jnp.zeros((facets, grid_size), jnp.int32)
    for f in range(facets):
        begins = jnp.where(f_rows == f, start_ref[f, mine], begins)
    ramp_cos, ramp_sin = sincos(
        ((begins * v_ids) & (grid_size - 1)).astype(jnp.float32) * (2.0 * math.pi / grid_size)
    )
    strip_total = strip_rows * owners * teams
    scale_col = 1.0 / math.sqrt(facets * grid_size) / math.sqrt(strip_total) / math.sqrt(grid_size)
    ramp_cos = ramp_cos * scale_col
    ramp_sin = ramp_sin * scale_col

    band = phase_ref.shape[0]
    block_v = LANES * RADIX
    from_ids = lax.broadcasted_iota(jnp.int32, (block_v, block_v), 0)
    to_ids = lax.broadcasted_iota(jnp.int32, (block_v, block_v), 1)
    chosen = (from_ids == (to_ids % LANES) * RADIX + to_ids // LANES).astype(jnp.float32).astype(jnp.bfloat16)
    for h in range(grid_size // block_v):
        whole = phase_ref[:, h * block_v : (h + 1) * block_v]
        ordered = jnp.zeros((band, block_v), jnp.float32)
        for level in range(3):
            digit = whole.astype(jnp.bfloat16)
            whole = whole - digit.astype(jnp.float32)
            ordered = ordered + jnp.dot(digit, chosen, preferred_element_type=jnp.float32)
        for p in range(RADIX):
            lanes = slice(p * part + h * LANES, p * part + (h + 1) * LANES)
            for l in range(cos_ref.shape[0]):
                level_value = level_ref[team_id * cos_ref.shape[0] + l].astype(jnp.float32)
                cos, sin = sincos(level_value * ordered[:, p * LANES : (p + 1) * LANES])
                cos_ref[l, :, lanes] = cos
                sin_ref[l, :, lanes] = sin

    for off in range(facets):
        for turn_o in range(owners):
            if off or turn_o:
                f = lax.rem(facet_id + off, facets)
                o = lax.rem(sub_id + turn_o, owners)
                pltpu.make_async_remote_copy(
                    src_ref=incoming.at[f, o],
                    dst_ref=incoming.at[f, o],
                    send_sem=pack_send.at[0],
                    recv_sem=pack_recv.at[f, o],
                    device_id=(f, o, team_id),
                    device_id_type=MESH,
                ).wait_recv()

    got = incoming[...].reshape(facets * owners * chunk, 2 * width).astype(jnp.float32)
    low_r, high_r = got[:, :part], got[:, part:width]
    low_i, high_i = got[:, width : width + part], got[:, width + part :]
    rows_f = owners * chunk
    images = [[], []]
    for p in range(RADIX):
        real, imag = [
            (low_r + high_r, low_i + high_i),
            (low_r - high_i, low_i + high_r),
            (low_r - high_r, low_i - high_i),
            (low_r + high_i, low_i - high_r),
        ][p]
        pair = jnp.concatenate([real.astype(jnp.bfloat16), imag.astype(jnp.bfloat16)], 1)
        moved = jnp.dot(pair, wide[p], preferred_element_type=jnp.float32)
        total_r = jnp.zeros((rows_f, part), jnp.float32)
        total_i = jnp.zeros((rows_f, part), jnp.float32)
        for f in range(facets):
            cos = ramp_cos[f : f + 1, p * part : (p + 1) * part]
            sin = ramp_sin[f : f + 1, p * part : (p + 1) * part]
            real = moved[f * rows_f : (f + 1) * rows_f, :part]
            imag = moved[f * rows_f : (f + 1) * rows_f, part:]
            total_r = total_r + (real * cos - imag * sin)
            total_i = total_i + (real * sin + imag * cos)
        images[0].append(total_r)
        images[1].append(total_i)
    piece_rows = 2 * rows_f // PARTS
    image = jnp.concatenate([jnp.concatenate(images[c], 1) for c in range(2)], 0).astype(jnp.bfloat16)
    for h in range(PARTS):
        gather_ref[facet_id, team_id, h] = image[h * piece_rows : (h + 1) * piece_rows]
    near_copy.wait()

    def send(kind, f, team, h, target):
        return pltpu.make_async_remote_copy(
            src_ref=gather_ref.at[f, team, h],
            dst_ref=gather_ref.at[f, team, h],
            send_sem=plane_send.at[kind, f, team // cores, h],
            recv_sem=block_recv.at[f, team, h],
            device_id=target,
            device_id_type=MESH,
        )

    def start(copy):
        copy.start()

    def finish_send(copy):
        copy.wait_send()

    def arrive(f, team, h):
        send(0, f, team, h, (facet_id, sub_id, team_id)).wait_recv()

    below = jnp.maximum(facet_id - 1, 0)
    above = jnp.minimum(facet_id + 1, facets - 1)

    def upward(f, h, act):
        @pl.when(facet_id < facets - 1)
        def _():
            act(send(0, f, team_id, h, (above, sub_id, team_id)))

    def downward(f, h, act):
        @pl.when(facet_id > 0)
        def _():
            act(send(1, f, team_id, h, (below, sub_id, team_id)))

    def across(f, h, act):
        for step in range(1, spread):
            act(send(1 + step, f, team_id, h, (facet_id, sub_id, team_at(step))))

    def aside(f, team, h, act):
        act(send(1 + spread, f, team, h, (facet_id, sub_id, sibling)))

    def from_below(d, h):
        @pl.when(facet_id >= d)
        def _():
            f = jnp.maximum(facet_id - d, 0)
            arrive(f, team_id, h)
            upward(f, h, start)
            across(f, h, start)
            aside(f, team_id, h, start)

    def from_above(d, h):
        @pl.when(facet_id < facets - d)
        def _():
            f = jnp.minimum(facet_id + d, facets - 1)
            arrive(f, team_id, h)
            downward(f, h, start)
            aside(f, team_id, h, start)
            if d > 1:
                across(f, h, start)
            else:
                pl.when(facet_id == 0)(lambda: across(f, h, start))

    def late_across(h):
        @pl.when((facet_id > 0) & (facet_id < facets - 1))
        def _():
            across(above, h, start)

    def partner(f, h):
        for step in range(1, spread):
            arrive(f, team_at(step), h)
            aside(f, team_at(step), h, start)

    def settled(f, h):
        for step in range(spread):
            arrive(f, lax.rem(sibling + cores * step, teams), h)

    def each_part(body):
        def run(h, carry):
            body(h)
            return carry

        lax.fori_loop(0, PARTS, run, 0)

    sequence = arrivals(facets, facet_id)
    early = facets - 1 if done_ref.shape[2] == cos_ref.shape[1] else 0

    def own(h):
        upward(facet_id, h, start)
        downward(facet_id, h, start)
        across(facet_id, h, start)
        aside(facet_id, team_id, h, start)

    each_part(own)

    def neighbours(h):
        from_below(1, h)
        from_above(1, h)
        partner(facet_id, h)

    each_part(neighbours)
    each_part(late_across)
    each_part(lambda h: settled(sequence[0], h))
    for k in range(facets - 1):

        def relay(h, k=k):
            if k + 2 < facets:
                from_below(k + 2, h)
                from_above(k + 2, h)
            partner(sequence[k + 1], h)
            if k < early:
                unit(h, gather_ref, sequence[k], near_ref, fwd_ref, cos_ref, sin_ref, held, done_ref.at[k])

        each_part(relay)
        each_part(lambda h, k=k: settled(sequence[k + 1], h))

    def drain(h):
        upward(facet_id, h, finish_send)
        downward(facet_id, h, finish_send)
        across(facet_id, h, finish_send)
        aside(facet_id, team_id, h, finish_send)
        for step in range(1, spread):
            aside(facet_id, team_at(step), h, finish_send)
        for d in range(1, facets):

            @pl.when(facet_id >= d)
            def _(d=d):
                f = jnp.maximum(facet_id - d, 0)
                upward(f, h, finish_send)
                across(f, h, finish_send)
                aside(f, team_id, h, finish_send)
                for step in range(1, spread):
                    aside(f, team_at(step), h, finish_send)

            @pl.when(facet_id < facets - d)
            def _(d=d):
                f = jnp.minimum(facet_id + d, facets - 1)
                downward(f, h, finish_send)
                across(f, h, finish_send)
                aside(f, team_id, h, finish_send)
                for step in range(1, spread):
                    aside(f, team_at(step), h, finish_send)

    each_part(drain)
    for copy, away in packs:
        if away is True:
            copy.wait_send()
        elif away is not None:
            pl.when(away)(copy.wait_send)


def column(scalars, sig, tables, left, phase, dims, layers, early):
    facets, owners, teams, strip_rows, facet_len, grid_size, slots, total_subs = dims
    first, twiddle, second, back = [jnp.asarray(x) for x in tables]
    group = facets // slots
    chunk = strip_rows // group
    width = grid_size // 2
    part = grid_size // RADIX
    band = phase.shape[0]
    smem = pl.BlockSpec(memory_space=pltpu.SMEM)
    vmem = pl.BlockSpec(memory_space=pltpu.VMEM)
    blocks = (facets, teams, PARTS, 2 * owners * chunk // PARTS, grid_size)
    spread = teams // 2
    return pl.pallas_call(
        functools.partial(column_kernel, dims),
        out_shape=[
            jax.ShapeDtypeStruct(blocks, jnp.bfloat16),
            jax.ShapeDtypeStruct((layers, band, grid_size), jnp.float32),
            jax.ShapeDtypeStruct((layers, band, grid_size), jnp.float32),
            jax.ShapeDtypeStruct(left.shape[1:], jnp.bfloat16),
            jax.ShapeDtypeStruct((RADIX, 2 * part, 2 * part), jnp.bfloat16),
            jax.ShapeDtypeStruct((max(early, 1), layers, band if early else 16, 2, grid_size), jnp.bfloat16),
        ],
        in_specs=[smem] * 6 + [vmem] * 6 + [pl.BlockSpec(memory_space=pl.ANY)],
        out_specs=[vmem] * 6,
        scratch_shapes=[
            pltpu.VMEM((strip_rows * (facet_len // LANES), 2 * LANES), jnp.bfloat16),
            pltpu.VMEM((2 * facet_len // LANES, strip_rows, LANES), jnp.float32),
            pltpu.VMEM((2, total_subs, 1, width), jnp.float32),
            pltpu.VMEM((facets * owners, chunk, 2 * width), jnp.bfloat16),
            pltpu.VMEM((facets, owners, chunk, 2 * width), jnp.bfloat16),
            pltpu.VMEM((RADIX, 2 * part, 2 * part), jnp.bfloat16),
            pltpu.VMEM((2 * band // HALVES, grid_size), jnp.bfloat16),
            pltpu.SemaphoreType.DMA((facets * owners,)),
            pltpu.SemaphoreType.DMA((facets, owners)),
            pltpu.SemaphoreType.DMA((2 + spread, facets, spread, PARTS)),
            pltpu.SemaphoreType.DMA((facets, teams, PARTS)),
            pltpu.SemaphoreType.DMA,
        ],
        compiler_params=pltpu.CompilerParams(
            collective_id=0, has_side_effects=True, vmem_limit_bytes=VMEM_COLUMN
        ),
        cost_estimate=pl.CostEstimate(flops=2_000_000_000, bytes_accessed=20_000_000, transcendentals=0),
    )(*scalars, sig, first, twiddle, second, back, phase, left)


def finish_kernel(early, facets, right_ref, cos_ref, sin_ref, near_ref, fwd_ref, done_ref, out_ref, held, ready, done_sem, ready_sem):
    layers, band, grid_size = cos_ref.shape
    slots = out_ref.shape[0]
    half = band // HALVES
    if early:
        sequence = arrivals(facets, lax.axis_index("facet"))
    else:
        sequence = list(range(slots))
    moved = []
    for k in range(early):
        moved.append(pltpu.make_async_copy(done_ref.at[k], out_ref.at[sequence[k]], done_sem.at[k]))
        moved[-1].start()

    def ship(slot, step):
        layer = lax.rem(step, layers)
        rows = pl.ds(pl.multiple_of(lax.div(step, layers) * half, half), half)
        return pltpu.make_async_copy(
            ready.at[layer, rows], out_ref.at[slot, layer, rows], ready_sem.at[step]
        )

    for k in range(early, slots):

        def run(step, carry, k=k):
            if k > early:
                ship(sequence[k - 1], step).wait()
            unit(step, right_ref, sequence[k], near_ref, fwd_ref, cos_ref, sin_ref, held, ready)
            ship(sequence[k], step).start()
            return carry

        lax.fori_loop(0, layers * HALVES, run, 0)
    for step in range(layers * HALVES):
        ship(sequence[slots - 1], step).wait()
    for copy in moved:
        copy.wait()


def finish(right, cos, sin, near, fwd, done, early, facets):
    layers, band, grid_size = cos.shape
    slots = right.shape[0]
    vmem = pl.BlockSpec(memory_space=pltpu.VMEM)
    return pl.pallas_call(
        functools.partial(finish_kernel, early, facets),
        out_shape=jax.ShapeDtypeStruct((slots, layers, band, 2, grid_size), jnp.bfloat16),
        in_specs=[vmem] * 6,
        out_specs=pl.BlockSpec(memory_space=pl.ANY),
        scratch_shapes=[
            pltpu.VMEM((2 * band // HALVES, grid_size), jnp.bfloat16),
            pltpu.VMEM((layers, band, 2, grid_size), jnp.bfloat16),
            pltpu.SemaphoreType.DMA((max(early, 1),)),
            pltpu.SemaphoreType.DMA((layers * HALVES,)),
        ],
        compiler_params=pltpu.CompilerParams(vmem_limit_bytes=VMEM_FINISH),
        cost_estimate=pl.CostEstimate(flops=2_000_000_000, bytes_accessed=20_000_000, transcendentals=0),
    )(right, cos, sin, near, fwd, done)


def local(
    facet_data,
    window,
    screen_phase,
    facet_shift,
    sub_offset,
    win_start,
    win_extent,
    owner_slot,
    layer_w,
):
    facets = lax.axis_size("facet")
    owners = lax.axis_size("sub")
    teams = lax.axis_size("wa")
    strip_rows = facet_data.shape[1]
    facet_len = facet_data.shape[3]
    band, grid_size = screen_phase.shape
    total_subs = owner_slot.shape[0]
    slots = total_subs // owners
    group = facets // slots
    chunk = strip_rows // group
    strip_total = strip_rows * owners * teams
    layers = layer_w.shape[0] // teams
    dims = (facets, owners, teams, strip_rows, facet_len, grid_size, slots, total_subs)

    outer_len = facet_len // LANES
    sig = (facet_data[0].astype(jnp.float32) * window).astype(jnp.bfloat16)
    sig = sig.reshape(strip_rows, 2 * outer_len, LANES)
    tables = strip_tables(facet_len, grid_size)
    scalars = (facet_shift, sub_offset, win_start, win_extent, owner_slot, layer_w)
    g_ids, t_ids, c_ids, o_ids, r_ids = np.meshgrid(
        np.arange(group), np.arange(teams), np.arange(2), np.arange(owners), np.arange(chunk), indexing="ij"
    )
    global_row = ((o_ids * teams + t_ids) * strip_rows + g_ids * chunk + r_ids).reshape(1, 1, -1)
    is_imag = c_ids.reshape(1, 1, -1)
    my_rows = np.arange(grid_size).reshape(facets * HALVES, band // HALVES, 1)
    all_cos, all_sin = table(my_rows * global_row, grid_size, -1.0)
    real_rows = np.where(is_imag == 1, -all_sin, all_cos)
    imag_rows = np.where(is_imag == 1, all_cos, all_sin)
    left = np.concatenate([real_rows, imag_rows], 1).astype(jnp.bfloat16)
    left = jnp.asarray(left.reshape(facets, HALVES, 2 * band // HALVES, 2 * strip_total))

    early = facets - 1 if group == 1 and layers * HALVES == PARTS else 0
    right, cos, sin, near, fwd, done = column(scalars, sig, tables, left, screen_phase, dims, layers, early)
    if not early:
        right = right.reshape(slots, 2 * strip_total, grid_size)
    return finish(right, cos, sin, near, fwd, done, early, facets)


def solution(mesh):
    in_specs = (
        P("facet", ("sub", "wa"), None, None),
        P(),
        P("facet", None),
        P(),
        P(),
        P(),
        P(),
        P(),
        P(),
    )
    out_specs = P("sub", "wa", "facet", None, None)
    return jax.shard_map(local, mesh=mesh, in_specs=in_specs, out_specs=out_specs, check_vma=False)
```

```python
import functools
import math

import jax
import jax.numpy as jnp
import numpy as np
from jax import lax
from jax.experimental import pallas as pl
from jax.experimental.pallas import tpu as pltpu
from jax.sharding import PartitionSpec as P

RADIX = 4
LANES = 128
PARTS = 4
HALVES = 2
VMEM_COLUMN = 32 * 1024 * 1024
VMEM_FINISH = 32 * 1024 * 1024
MESH = pl.DeviceIdType.MESH


def table(products, modulus, sign_value):
    angles = (sign_value * 2.0 * math.pi / modulus) * (products % modulus).astype(np.float64)
    return np.cos(angles), np.sin(angles)


def sincos(angles):
    turns = jnp.floor(angles * (2.0 / math.pi) + 0.5)
    rest = angles - turns * 1.5703125
    rest = rest - turns * 4.837512969970703e-4
    rest = rest - turns * 7.549789948768648e-8
    square = rest * rest
    sine = rest + rest * square * (
        -1.6666654611e-1 + square * (8.3321608736e-3 + square * -1.9515295891e-4)
    )
    cosine = (1.0 - 0.5 * square) + square * square * (
        4.166664568298827e-2 + square * (-1.388731625493765e-3 + square * 2.443315711809948e-5)
    )
    quadrant = turns.astype(jnp.int32)
    odd = (quadrant & 1) == 1
    sin_size = jnp.where(odd, cosine, sine)
    cos_size = jnp.where(odd, sine, cosine)
    sin_value = jnp.where((quadrant & 2) == 2, -sin_size, sin_size)
    cos_value = jnp.where(((quadrant + 1) & 2) == 2, -cos_size, cos_size)
    return cos_value, sin_value


def strip_tables(facet_len, grid_size):
    inner_len = LANES
    outer_len = facet_len // inner_len
    outer_ids = np.arange(outer_len)
    inner_ids = np.arange(inner_len)
    c1, s1 = table(outer_ids[:, None] * outer_ids[None, :], outer_len, -1.0)
    first = np.block([[c1, -s1], [s1, c1]])
    first = first.reshape(-1, 2, outer_len).transpose(0, 2, 1).reshape(-1, 2 * outer_len).astype(jnp.bfloat16)
    ct, st = table(outer_ids[:, None] * inner_ids[None, :], facet_len, -1.0)
    twiddle = np.stack([ct, st]).astype(np.float32)
    fold = LANES // outer_len
    q_ids = (np.arange(inner_len // fold)[None, :] * fold + np.arange(fold)[:, None]).reshape(-1)
    c2, s2 = table(q_ids[:, None] * inner_ids[None, :], inner_len, -1.0)
    scale = 1.0 / math.sqrt(facet_len)
    second = (np.block([[c2, -s2], [s2, c2]]) * scale).astype(jnp.bfloat16)
    part = grid_size // RADIX
    v_ids = np.arange(part)[None, :] * RADIX + np.arange(RADIX)[:, None]
    bc, bs = table(np.arange(part)[None, :, None] * v_ids[:, None, :], grid_size, 1.0)
    back = np.concatenate([bc, bs], 2).astype(jnp.bfloat16)
    return first, twiddle, second, back


def arrivals(facets, facet_id):
    order = []
    for z in range(facets):
        row = [z]
        for d in range(1, facets):
            row += [f for f in (z - d, z + d) if 0 <= f < facets]
        order.append(row)
    picked = []
    for k in range(facets):
        value = 0
        for z in range(facets):
            gap = facet_id - z
            here = 1 - lax.div(gap * gap + (facets * facets - 1), facets * facets)
            value = value + here * order[z][k]
        picked.append(value)
    return picked


def unit(step, right_ref, slot, near_ref, fwd_ref, cos_ref, sin_ref, held, out_ref):
    layers, band, grid_size = cos_ref.shape
    part = grid_size // RADIX
    half = band // HALVES
    layer = lax.rem(step, layers)
    which = lax.div(step, layers)
    rows = pl.ds(pl.multiple_of(which * half, half), half)

    @pl.when(layer == 0)
    def _():
        right = right_ref[slot].reshape(near_ref.shape[2], grid_size)
        for p in range(RADIX):
            lanes = slice(p * part, (p + 1) * part)
            got = jnp.dot(near_ref[which], right[:, lanes], preferred_element_type=jnp.float32)
            held[:, lanes] = got.astype(jnp.bfloat16)

    pieces = []
    for p in range(RADIX):
        lanes = slice(p * part, (p + 1) * part)
        real = held[:half, lanes].astype(jnp.float32)
        imag = held[half:, lanes].astype(jnp.float32)
        cos = cos_ref[layer, rows, lanes]
        sin = sin_ref[layer, rows, lanes]
        s_real = (real * cos - imag * sin).astype(jnp.bfloat16)
        s_imag = (real * sin + imag * cos).astype(jnp.bfloat16)
        pair = jnp.concatenate([s_real, s_imag], 1)
        got = jnp.dot(pair, fwd_ref[p], preferred_element_type=jnp.float32)
        pieces.append((got[:, :part], got[:, part:]))
    (ar, ai), (br, bi), (cr, ci), (dr, di) = pieces
    er, ei, fr, fi = ar + cr, ai + ci, ar - cr, ai - ci
    gr, gi, hr, hi_ = br + dr, bi + di, br - dr, bi - di
    reals = jnp.concatenate([er + gr, fr + hi_, er - gr, fr - hi_], 1)
    imags = jnp.concatenate([ei + gi, fi - hr, ei - gi, fi + hr], 1)
    out_ref[layer, rows, 0, :] = reals.astype(jnp.bfloat16)
    out_ref[layer, rows, 1, :] = imags.astype(jnp.bfloat16)


def column_kernel(dims, *refs):
    sources = refs[:14]
    gather_ref, cos_ref, sin_ref, near_ref, fwd_ref, done_ref = refs[14:20]
    (
        shift_ref,
        offset_ref,
        start_ref,
        extent_ref,
        slot_ref,
        level_ref,
        sig_ref,
        shade_ref,
        first_ref,
        twiddle_ref,
        second_ref,
        back_ref,
        phase_ref,
    ) = refs[20:33]
    weights, mid, spec, turn, outgoing, incoming, wide, held = refs[33:41]
    pack_send, pack_recv, plane_send, block_recv, load_sem = refs[41:]
    loads = [
        pltpu.make_async_copy(source, target, load_sem.at[n])
        for n, (source, target) in enumerate(zip(sources, refs[20:33]))
    ]
    loads.append(pltpu.make_async_copy(sources[13].at[lax.axis_index("facet")], near_ref, load_sem.at[13]))
    order = [6, 7, 8, 9, 10, 0, 1, 2, 3, 4, 5, 11, 12, 13]
    for n in order:
        loads[n].start()
    facets, owners, teams, strip_rows, facet_len, grid_size, slots, total_subs = dims
    facet_id = lax.axis_index("facet")
    sub_id = lax.axis_index("sub")
    team_id = lax.axis_index("wa")
    group = facets // slots
    chunk = strip_rows // group
    width = grid_size // 2
    part = grid_size // RADIX
    cores = 2
    spread = teams // cores
    core_id = lax.rem(team_id, cores)
    sibling = team_id + 1 - 2 * core_id

    def team_at(step):
        return lax.rem(team_id + cores * step, teams)

    barrier = pltpu.get_barrier_semaphore()
    peers = 0
    for off in range(facets):
        for turn_o in range(owners):
            if off or turn_o:
                pl.semaphore_signal(
                    barrier,
                    inc=1,
                    device_id=(lax.rem(facet_id + off, facets), lax.rem(sub_id + turn_o, owners), team_id),
                    device_id_type=MESH,
                )
                peers += 1
    for step in range(1, spread):
        pl.semaphore_signal(
            barrier, inc=1, device_id=(facet_id, sub_id, team_at(step)), device_id_type=MESH
        )
        peers += 1
    pl.semaphore_signal(barrier, inc=1, device_id=(facet_id, sub_id, sibling), device_id_type=MESH)
    peers += 1

    def holder(slot):
        def look(j, found):
            return jnp.where(slot_ref[j] == slot, j, found)

        return lax.fori_loop(0, total_subs, look, jnp.int32(0))

    outer_len = facet_len // LANES
    fold = LANES // outer_len
    for n in order[:5]:
        loads[n].wait()
    tw_cos = twiddle_ref[0]
    tw_sin = twiddle_ref[1]

    for c in range(2):
        weights[pl.ds(c, outer_len, stride=2), :] = shade_ref[...]

    def first_step(r, carry):
        signal = sig_ref[r].reshape(2 * outer_len, LANES).astype(jnp.float32) * weights[...]
        got = jnp.dot(first_ref[...], signal.astype(jnp.bfloat16), preferred_element_type=jnp.float32)
        real, imag = got[:outer_len], got[outer_len:]
        rows = pl.ds(pl.multiple_of(r * outer_len, outer_len), outer_len)
        mid[rows, :LANES] = (real * tw_cos - imag * tw_sin).astype(jnp.bfloat16)
        mid[rows, LANES:] = (real * tw_sin + imag * tw_cos).astype(jnp.bfloat16)
        return carry

    lax.fori_loop(0, strip_rows, first_step, 0)
    tall = LANES // fold
    lane = lax.broadcasted_iota(jnp.int32, (tall, LANES), 1)

    def second_step(i, carry):
        rows = pl.ds(pl.multiple_of(i * LANES, LANES), LANES)
        got = lax.dot_general(
            second_ref[...], mid[rows, :], (((1,), (1,)), ((), ())), preferred_element_type=jnp.float32
        )
        for c in range(2):
            even = got[c * LANES : c * LANES + tall]
            odd = got[c * LANES + tall : (c + 1) * LANES]
            near = jnp.where(lane < outer_len, even, pltpu.roll(odd, outer_len, 1))
            far = jnp.where(lane < outer_len, pltpu.roll(even, outer_len, 1), odd)
            spec[c * tall : (c + 1) * tall, i * fold, :] = near
            spec[c * tall : (c + 1) * tall, i * fold + 1, :] = far
        return carry

    lax.fori_loop(0, strip_rows // fold, second_step, 0)

    for n in range(6):
        loads[n].wait()
    holders = [holder(p) for p in range(total_subs)]
    row_ids = lax.broadcasted_iota(jnp.int32, (total_subs, width), 0)
    k_ids = lax.broadcasted_iota(jnp.int32, (total_subs, width), 1)
    starts = jnp.zeros((total_subs, width), jnp.int32)
    extents = jnp.zeros((total_subs, width), jnp.int32)
    for p in range(total_subs):
        starts = jnp.where(row_ids == p, start_ref[facet_id, holders[p]], starts)
        extents = jnp.where(row_ids == p, extent_ref[facet_id, holders[p]], extents)
    product = (shift_ref[facet_id] * (starts + k_ids)) & (grid_size - 1)
    turn_cos, turn_sin = sincos(product.astype(jnp.float32) * (2.0 * math.pi / grid_size))
    inside = k_ids < extents
    turn_cos = jnp.where(inside, turn_cos, 0.0)
    turn_sin = jnp.where(inside, turn_sin, 0.0)
    for p in range(total_subs):
        turn[0, p] = turn_cos[p : p + 1]
        turn[1, p] = turn_sin[p : p + 1]

    pl.semaphore_wait(barrier, peers)

    wide_lane = lax.broadcasted_iota(jnp.int32, (strip_rows, LANES), 1)
    pieces = width // LANES
    my_slot = facet_id // group
    packs = []
    steps = [s for s in range(slots // 2, slots)] + [s for s in range(slots // 2)][::-1]
    for step in steps:
        for turn_o in list(range(1, owners)) + [0]:
            slot = lax.rem(my_slot + step, slots)
            owner = lax.rem(sub_id + turn_o, owners)
            p = owner * slots + slot
            j = holder(p)
            begin = lax.rem(offset_ref[j] + start_ref[facet_id, j], facet_len)
            q0 = lax.div(begin, LANES)
            shift = begin - q0 * LANES
            back_by = lax.rem(LANES - shift, LANES)
            tiles = []
            for c in range(2):
                rolled = []
                for q in range(pieces + 1):
                    tile = spec[c * tall + lax.rem(q0 + q, tall)]
                    rolled.append(pltpu.roll(tile, back_by, 1))
                tiles.append(
                    [jnp.where(wide_lane < LANES - shift, rolled[q], rolled[q + 1]) for q in range(pieces)]
                )
            reals, imags = [], []
            for q in range(pieces):
                lanes = slice(q * LANES, (q + 1) * LANES)
                cos = turn[0, p, :, lanes]
                sin = turn[1, p, :, lanes]
                reals.append(tiles[0][q] * cos - tiles[1][q] * sin)
                imags.append(tiles[0][q] * sin + tiles[1][q] * cos)
            block = jnp.concatenate(reals + imags, 1).astype(jnp.bfloat16)
            for g in range(group):
                target = slot * group + g
                piece = block[g * chunk : (g + 1) * chunk]
                n = len(packs)
                outgoing[n] = piece
                here = group == 1 and step == 0 and turn_o == 0
                if here:
                    incoming[facet_id, sub_id] = piece
                    packs.append((None, None))
                    continue
                copy = pltpu.make_async_remote_copy(
                    src_ref=outgoing.at[n],
                    dst_ref=incoming.at[facet_id, sub_id],
                    send_sem=pack_send.at[n],
                    recv_sem=pack_recv.at[facet_id, sub_id],
                    device_id=(target, owner, team_id),
                    device_id_type=MESH,
                )
                if step == 0 and turn_o == 0:
                    away = target != facet_id
                    pl.when(away)(copy.start)

                    @pl.when(target == facet_id)
                    def _():
                        incoming[facet_id, sub_id] = piece

                    packs.append((copy, away))
                else:
                    copy.start()
                    packs.append((copy, True))

    loads[11].wait()
    loads[12].wait()
    for p in range(RADIX):
        wide[p, :part] = back_ref[p]
        wide[p, part:, :part] = -back_ref[p][:, part:]
        wide[p, part:, part:] = back_ref[p][:, :part]
        fwd_ref[p] = wide[p].T
    mine = holder(sub_id * slots + my_slot)
    f_rows = lax.broadcasted_iota(jnp.int32, (facets, grid_size), 0)
    at = lax.broadcasted_iota(jnp.int32, (facets, grid_size), 1)
    v_ids = (at % part) * RADIX + at // part
    begins = jnp.zeros((facets, grid_size), jnp.int32)
    for f in range(facets):
        begins = jnp.where(f_rows == f, start_ref[f, mine], begins)
    ramp_cos, ramp_sin = sincos(
        ((begins * v_ids) & (grid_size - 1)).astype(jnp.float32) * (2.0 * math.pi / grid_size)
    )
    strip_total = strip_rows * owners * teams
    scale_col = 1.0 / math.sqrt(facets * grid_size) / math.sqrt(strip_total) / math.sqrt(grid_size)
    ramp_cos = ramp_cos * scale_col
    ramp_sin = ramp_sin * scale_col

    band = phase_ref.shape[0]
    block_v = LANES * RADIX
    from_ids = lax.broadcasted_iota(jnp.int32, (block_v, block_v), 0)
    to_ids = lax.broadcasted_iota(jnp.int32, (block_v, block_v), 1)
    chosen = (from_ids == (to_ids % LANES) * RADIX + to_ids // LANES).astype(jnp.float32).astype(jnp.bfloat16)
    for h in range(grid_size // block_v):
        whole = phase_ref[:, h * block_v : (h + 1) * block_v]
        ordered = jnp.zeros((band, block_v), jnp.float32)
        for level in range(3):
            digit = whole.astype(jnp.bfloat16)
            whole = whole - digit.astype(jnp.float32)
            ordered = ordered + jnp.dot(digit, chosen, preferred_element_type=jnp.float32)
        for p in range(RADIX):
            lanes = slice(p * part + h * LANES, p * part + (h + 1) * LANES)
            for l in range(cos_ref.shape[0]):
                level_value = level_ref[team_id * cos_ref.shape[0] + l].astype(jnp.float32)
                cos, sin = sincos(level_value * ordered[:, p * LANES : (p + 1) * LANES])
                cos_ref[l, :, lanes] = cos
                sin_ref[l, :, lanes] = sin

    for off in range(facets):
        for turn_o in range(owners):
            if off or turn_o:
                f = lax.rem(facet_id + off, facets)
                o = lax.rem(sub_id + turn_o, owners)
                pltpu.make_async_remote_copy(
                    src_ref=incoming.at[f, o],
                    dst_ref=incoming.at[f, o],
                    send_sem=pack_send.at[0],
                    recv_sem=pack_recv.at[f, o],
                    device_id=(f, o, team_id),
                    device_id_type=MESH,
                ).wait_recv()

    got = incoming[...].reshape(facets * owners * chunk, 2 * width).astype(jnp.float32)
    low_r, high_r = got[:, :part], got[:, part:width]
    low_i, high_i = got[:, width : width + part], got[:, width + part :]
    rows_f = owners * chunk
    images = [[], []]
    for p in range(RADIX):
        real, imag = [
            (low_r + high_r, low_i + high_i),
            (low_r - high_i, low_i + high_r),
            (low_r - high_r, low_i - high_i),
            (low_r + high_i, low_i - high_r),
        ][p]
        pair = jnp.concatenate([real.astype(jnp.bfloat16), imag.astype(jnp.bfloat16)], 1)
        moved = jnp.dot(pair, wide[p], preferred_element_type=jnp.float32)
        total_r = jnp.zeros((rows_f, part), jnp.float32)
        total_i = jnp.zeros((rows_f, part), jnp.float32)
        for f in range(facets):
            cos = ramp_cos[f : f + 1, p * part : (p + 1) * part]
            sin = ramp_sin[f : f + 1, p * part : (p + 1) * part]
            real = moved[f * rows_f : (f + 1) * rows_f, :part]
            imag = moved[f * rows_f : (f + 1) * rows_f, part:]
            total_r = total_r + (real * cos - imag * sin)
            total_i = total_i + (real * sin + imag * cos)
        images[0].append(total_r)
        images[1].append(total_i)
    piece_rows = 2 * rows_f // PARTS
    image = jnp.concatenate([jnp.concatenate(images[c], 1) for c in range(2)], 0).astype(jnp.bfloat16)
    for h in range(PARTS):
        gather_ref[facet_id, team_id, h] = image[h * piece_rows : (h + 1) * piece_rows]
    loads[13].wait()

    def send(kind, f, team, h, target):
        return pltpu.make_async_remote_copy(
            src_ref=gather_ref.at[f, team, h],
            dst_ref=gather_ref.at[f, team, h],
            send_sem=plane_send.at[kind, f, team // cores, h],
            recv_sem=block_recv.at[f, team, h],
            device_id=target,
            device_id_type=MESH,
        )

    def start(copy):
        copy.start()

    def finish_send(copy):
        copy.wait_send()

    def arrive(f, team, h):
        send(0, f, team, h, (facet_id, sub_id, team_id)).wait_recv()

    below = jnp.maximum(facet_id - 1, 0)
    above = jnp.minimum(facet_id + 1, facets - 1)

    def upward(f, h, act):
        @pl.when(facet_id < facets - 1)
        def _():
            act(send(0, f, team_id, h, (above, sub_id, team_id)))

    def downward(f, h, act):
        @pl.when(facet_id > 0)
        def _():
            act(send(1, f, team_id, h, (below, sub_id, team_id)))

    def across(f, h, act):
        for step in range(1, spread):
            act(send(1 + step, f, team_id, h, (facet_id, sub_id, team_at(step))))

    def aside(f, team, h, act):
        act(send(1 + spread, f, team, h, (facet_id, sub_id, sibling)))

    def from_below(d, h):
        @pl.when(facet_id >= d)
        def _():
            f = jnp.maximum(facet_id - d, 0)
            arrive(f, team_id, h)
            upward(f, h, start)
            across(f, h, start)
            aside(f, team_id, h, start)

    def from_above(d, h):
        @pl.when(facet_id < facets - d)
        def _():
            f = jnp.minimum(facet_id + d, facets - 1)
            arrive(f, team_id, h)
            downward(f, h, start)
            aside(f, team_id, h, start)
            if d > 1:
                across(f, h, start)
            else:
                pl.when(facet_id == 0)(lambda: across(f, h, start))

    def late_across(h):
        @pl.when((facet_id > 0) & (facet_id < facets - 1))
        def _():
            across(above, h, start)

    def partner(f, h):
        for step in range(1, spread):
            arrive(f, team_at(step), h)
            aside(f, team_at(step), h, start)

    def settled(f, h):
        for step in range(spread):
            arrive(f, lax.rem(sibling + cores * step, teams), h)

    def each_part(body):
        def run(h, carry):
            body(h)
            return carry

        lax.fori_loop(0, PARTS, run, 0)

    sequence = arrivals(facets, facet_id)
    early = facets - 1 if done_ref.shape[2] == cos_ref.shape[1] else 0

    def own(h):
        upward(facet_id, h, start)
        downward(facet_id, h, start)
        across(facet_id, h, start)
        aside(facet_id, team_id, h, start)

    each_part(own)

    def neighbours(h):
        from_below(1, h)
        from_above(1, h)
        partner(facet_id, h)

    each_part(neighbours)
    each_part(late_across)
    each_part(lambda h: settled(sequence[0], h))
    for k in range(facets - 1):

        def relay(h, k=k):
            if k + 2 < facets:
                from_below(k + 2, h)
                from_above(k + 2, h)
            partner(sequence[k + 1], h)
            if k < early:
                unit(h, gather_ref, sequence[k], near_ref, fwd_ref, cos_ref, sin_ref, held, done_ref.at[k])

        each_part(relay)
        each_part(lambda h, k=k: settled(sequence[k + 1], h))

    def drain(h):
        upward(facet_id, h, finish_send)
        downward(facet_id, h, finish_send)
        across(facet_id, h, finish_send)
        aside(facet_id, team_id, h, finish_send)
        for step in range(1, spread):
            aside(facet_id, team_at(step), h, finish_send)
        for d in range(1, facets):

            @pl.when(facet_id >= d)
            def _(d=d):
                f = jnp.maximum(facet_id - d, 0)
                upward(f, h, finish_send)
                across(f, h, finish_send)
                aside(f, team_id, h, finish_send)
                for step in range(1, spread):
                    aside(f, team_at(step), h, finish_send)

            @pl.when(facet_id < facets - d)
            def _(d=d):
                f = jnp.minimum(facet_id + d, facets - 1)
                downward(f, h, finish_send)
                across(f, h, finish_send)
                aside(f, team_id, h, finish_send)
                for step in range(1, spread):
                    aside(f, team_at(step), h, finish_send)

    each_part(drain)
    for copy, away in packs:
        if away is True:
            copy.wait_send()
        elif away is not None:
            pl.when(away)(copy.wait_send)


def column(scalars, sig, shade, tables, left, phase, dims, layers, early):
    facets, owners, teams, strip_rows, facet_len, grid_size, slots, total_subs = dims
    first, twiddle, second, back = [jnp.asarray(x) for x in tables]
    group = facets // slots
    chunk = strip_rows // group
    width = grid_size // 2
    part = grid_size // RADIX
    band = phase.shape[0]
    hbm = pl.BlockSpec(memory_space=pltpu.HBM)
    vmem = pl.BlockSpec(memory_space=pltpu.VMEM)
    operands = [*scalars, sig, shade, first, twiddle, second, back, phase]
    blocks = (facets, teams, PARTS, 2 * owners * chunk // PARTS, grid_size)
    spread = teams // 2
    return pl.pallas_call(
        functools.partial(column_kernel, dims),
        out_shape=[
            jax.ShapeDtypeStruct(blocks, jnp.bfloat16),
            jax.ShapeDtypeStruct((layers, band, grid_size), jnp.float32),
            jax.ShapeDtypeStruct((layers, band, grid_size), jnp.float32),
            jax.ShapeDtypeStruct(left.shape[1:], jnp.bfloat16),
            jax.ShapeDtypeStruct((RADIX, 2 * part, 2 * part), jnp.bfloat16),
            jax.ShapeDtypeStruct((max(early, 1), layers, band if early else 16, 2, grid_size), jnp.bfloat16),
        ],
        in_specs=[hbm] * 14,
        out_specs=[vmem] * 6,
        scratch_shapes=[pltpu.SMEM(x.shape, x.dtype) for x in operands[:6]]
        + [pltpu.VMEM(x.shape, x.dtype) for x in operands[6:]]
        + [
            pltpu.VMEM((2 * facet_len // LANES, LANES), jnp.float32),
            pltpu.VMEM((strip_rows * (facet_len // LANES), 2 * LANES), jnp.bfloat16),
            pltpu.VMEM((2 * facet_len // LANES, strip_rows, LANES), jnp.float32),
            pltpu.VMEM((2, total_subs, 1, width), jnp.float32),
            pltpu.VMEM((facets * owners, chunk, 2 * width), jnp.bfloat16),
            pltpu.VMEM((facets, owners, chunk, 2 * width), jnp.bfloat16),
            pltpu.VMEM((RADIX, 2 * part, 2 * part), jnp.bfloat16),
            pltpu.VMEM((2 * band // HALVES, grid_size), jnp.bfloat16),
            pltpu.SemaphoreType.DMA((facets * owners,)),
            pltpu.SemaphoreType.DMA((facets, owners)),
            pltpu.SemaphoreType.DMA((2 + spread, facets, spread, PARTS)),
            pltpu.SemaphoreType.DMA((facets, teams, PARTS)),
            pltpu.SemaphoreType.DMA((14,)),
        ],
        compiler_params=pltpu.CompilerParams(
            collective_id=0, has_side_effects=True, vmem_limit_bytes=VMEM_COLUMN
        ),
        cost_estimate=pl.CostEstimate(flops=2_000_000_000, bytes_accessed=20_000_000, transcendentals=0),
    )(*[pltpu.with_memory_space_constraint(x, pltpu.HBM) for x in operands + [left]])


def finish_kernel(early, facets, right_ref, cos_ref, sin_ref, near_ref, fwd_ref, done_ref, out_ref, held, ready, done_sem, ready_sem):
    layers, band, grid_size = cos_ref.shape
    slots = out_ref.shape[0]
    half = band // HALVES
    if early:
        sequence = arrivals(facets, lax.axis_index("facet"))
    else:
        sequence = list(range(slots))
    moved = []
    for k in range(early):
        moved.append(pltpu.make_async_copy(done_ref.at[k], out_ref.at[sequence[k]], done_sem.at[k]))
        moved[-1].start()

    def ship(slot, step):
        layer = lax.rem(step, layers)
        rows = pl.ds(pl.multiple_of(lax.div(step, layers) * half, half), half)
        return pltpu.make_async_copy(
            ready.at[layer, rows], out_ref.at[slot, layer, rows], ready_sem.at[step]
        )

    for k in range(early, slots):

        def run(step, carry, k=k):
            if k > early:
                ship(sequence[k - 1], step).wait()
            unit(step, right_ref, sequence[k], near_ref, fwd_ref, cos_ref, sin_ref, held, ready)
            ship(sequence[k], step).start()
            return carry

        lax.fori_loop(0, layers * HALVES, run, 0)
    for step in range(layers * HALVES):
        ship(sequence[slots - 1], step).wait()
    for copy in moved:
        copy.wait()


def finish(right, cos, sin, near, fwd, done, early, facets):
    layers, band, grid_size = cos.shape
    slots = right.shape[0]
    vmem = pl.BlockSpec(memory_space=pltpu.VMEM)
    return pl.pallas_call(
        functools.partial(finish_kernel, early, facets),
        out_shape=jax.ShapeDtypeStruct((slots, layers, band, 2, grid_size), jnp.bfloat16),
        in_specs=[vmem] * 6,
        out_specs=pl.BlockSpec(memory_space=pl.ANY),
        scratch_shapes=[
            pltpu.VMEM((2 * band // HALVES, grid_size), jnp.bfloat16),
            pltpu.VMEM((layers, band, 2, grid_size), jnp.bfloat16),
            pltpu.SemaphoreType.DMA((max(early, 1),)),
            pltpu.SemaphoreType.DMA((layers * HALVES,)),
        ],
        compiler_params=pltpu.CompilerParams(vmem_limit_bytes=VMEM_FINISH),
        cost_estimate=pl.CostEstimate(flops=2_000_000_000, bytes_accessed=20_000_000, transcendentals=0),
    )(right, cos, sin, near, fwd, done)


def local(
    facet_data,
    window,
    screen_phase,
    facet_shift,
    sub_offset,
    win_start,
    win_extent,
    owner_slot,
    layer_w,
):
    facets = lax.axis_size("facet")
    owners = lax.axis_size("sub")
    teams = lax.axis_size("wa")
    strip_rows = facet_data.shape[1]
    facet_len = facet_data.shape[3]
    band, grid_size = screen_phase.shape
    total_subs = owner_slot.shape[0]
    slots = total_subs // owners
    group = facets // slots
    chunk = strip_rows // group
    strip_total = strip_rows * owners * teams
    layers = layer_w.shape[0] // teams
    dims = (facets, owners, teams, strip_rows, facet_len, grid_size, slots, total_subs)

    outer_len = facet_len // LANES
    sig = facet_data[0].reshape(strip_rows, 2, outer_len, LANES).transpose(0, 2, 1, 3)
    shade = window.reshape(outer_len, LANES)
    tables = strip_tables(facet_len, grid_size)
    scalars = (facet_shift, sub_offset, win_start, win_extent, owner_slot, layer_w)
    g_ids, t_ids, c_ids, o_ids, r_ids = np.meshgrid(
        np.arange(group), np.arange(teams), np.arange(2), np.arange(owners), np.arange(chunk), indexing="ij"
    )
    global_row = ((o_ids * teams + t_ids) * strip_rows + g_ids * chunk + r_ids).reshape(1, 1, -1)
    is_imag = c_ids.reshape(1, 1, -1)
    my_rows = np.arange(grid_size).reshape(facets * HALVES, band // HALVES, 1)
    all_cos, all_sin = table(my_rows * global_row, grid_size, -1.0)
    real_rows = np.where(is_imag == 1, -all_sin, all_cos)
    imag_rows = np.where(is_imag == 1, all_cos, all_sin)
    left = np.concatenate([real_rows, imag_rows], 1).astype(jnp.bfloat16)
    left = jnp.asarray(left.reshape(facets, HALVES, 2 * band // HALVES, 2 * strip_total))

    early = facets - 1 if group == 1 and layers * HALVES == PARTS else 0
    right, cos, sin, near, fwd, done = column(scalars, sig, shade, tables, left, screen_phase, dims, layers, early)
    if not early:
        right = right.reshape(slots, 2 * strip_total, grid_size)
    return finish(right, cos, sin, near, fwd, done, early, facets)


def solution(mesh):
    in_specs = (
        P("facet", ("sub", "wa"), None, None),
        P(),
        P("facet", None),
        P(),
        P(),
        P(),
        P(),
        P(),
        P(),
    )
    out_specs = P("sub", "wa", "facet", None, None)
    return jax.shard_map(local, mesh=mesh, in_specs=in_specs, out_specs=out_specs, check_vma=False)
```

```python
import functools
import math

import jax
import jax.numpy as jnp
import numpy as np
from jax import lax
from jax.experimental import pallas as pl
from jax.experimental.pallas import tpu as pltpu
from jax.sharding import PartitionSpec as P

RADIX = 4
LANES = 128
PARTS = 4
HALVES = 2
VMEM_COLUMN = 32 * 1024 * 1024
VMEM_FINISH = 32 * 1024 * 1024
MESH = pl.DeviceIdType.MESH


def table(products, modulus, sign_value):
    angles = (sign_value * 2.0 * math.pi / modulus) * (products % modulus).astype(np.float64)
    return np.cos(angles), np.sin(angles)


def sincos(angles):
    turns = jnp.floor(angles * (2.0 / math.pi) + 0.5)
    rest = angles - turns * 1.5703125
    rest = rest - turns * 4.837512969970703e-4
    rest = rest - turns * 7.549789948768648e-8
    square = rest * rest
    sine = rest + rest * square * (
        -1.6666654611e-1 + square * (8.3321608736e-3 + square * -1.9515295891e-4)
    )
    cosine = (1.0 - 0.5 * square) + square * square * (
        4.166664568298827e-2 + square * (-1.388731625493765e-3 + square * 2.443315711809948e-5)
    )
    quadrant = turns.astype(jnp.int32)
    odd = (quadrant & 1) == 1
    sin_size = jnp.where(odd, cosine, sine)
    cos_size = jnp.where(odd, sine, cosine)
    sin_value = jnp.where((quadrant & 2) == 2, -sin_size, sin_size)
    cos_value = jnp.where(((quadrant + 1) & 2) == 2, -cos_size, cos_size)
    return cos_value, sin_value


def strip_tables(facet_len, grid_size):
    inner_len = LANES
    outer_len = facet_len // inner_len
    outer_ids = np.arange(outer_len)
    inner_ids = np.arange(inner_len)
    c1, s1 = table(outer_ids[:, None] * outer_ids[None, :], outer_len, -1.0)
    first = np.block([[c1, -s1], [s1, c1]])
    first = first.reshape(-1, 2, outer_len).transpose(0, 2, 1).reshape(-1, 2 * outer_len).astype(jnp.bfloat16)
    ct, st = table(outer_ids[:, None] * inner_ids[None, :], facet_len, -1.0)
    twiddle = np.stack([ct, st]).astype(np.float32)
    fold = LANES // outer_len
    q_ids = (np.arange(inner_len // fold)[None, :] * fold + np.arange(fold)[:, None]).reshape(-1)
    c2, s2 = table(q_ids[:, None] * inner_ids[None, :], inner_len, -1.0)
    scale = 1.0 / math.sqrt(facet_len)
    second = (np.block([[c2, -s2], [s2, c2]]) * scale).astype(jnp.bfloat16)
    part = grid_size // RADIX
    v_ids = np.arange(part)[None, :] * RADIX + np.arange(RADIX)[:, None]
    bc, bs = table(np.arange(part)[None, :, None] * v_ids[:, None, :], grid_size, 1.0)
    back = np.concatenate([bc, bs], 2).astype(jnp.bfloat16)
    return first, twiddle, second, back


def arrivals(facets, facet_id):
    order = []
    for z in range(facets):
        row = [z]
        for d in range(1, facets):
            row += [f for f in (z - d, z + d) if 0 <= f < facets]
        order.append(row)
    picked = []
    for k in range(facets):
        value = 0
        for z in range(facets):
            gap = facet_id - z
            here = 1 - lax.div(gap * gap + (facets * facets - 1), facets * facets)
            value = value + here * order[z][k]
        picked.append(value)
    return picked


def unit(step, right_ref, slot, near_ref, fwd_ref, cos_ref, sin_ref, held, out_ref):
    layers, band, grid_size = cos_ref.shape
    part = grid_size // RADIX
    half = band // HALVES
    layer = lax.rem(step, layers)
    which = lax.div(step, layers)
    rows = pl.ds(pl.multiple_of(which * half, half), half)

    @pl.when(layer == 0)
    def _():
        right = right_ref[slot].reshape(near_ref.shape[2], grid_size)
        for p in range(RADIX):
            lanes = slice(p * part, (p + 1) * part)
            got = jnp.dot(near_ref[which], right[:, lanes], preferred_element_type=jnp.float32)
            held[:, lanes] = got.astype(jnp.bfloat16)

    pieces = []
    for p in range(RADIX):
        lanes = slice(p * part, (p + 1) * part)
        real = held[:half, lanes].astype(jnp.float32)
        imag = held[half:, lanes].astype(jnp.float32)
        cos = cos_ref[layer, rows, lanes]
        sin = sin_ref[layer, rows, lanes]
        s_real = (real * cos - imag * sin).astype(jnp.bfloat16)
        s_imag = (real * sin + imag * cos).astype(jnp.bfloat16)
        pair = jnp.concatenate([s_real, s_imag], 1)
        got = jnp.dot(pair, fwd_ref[p], preferred_element_type=jnp.float32)
        pieces.append((got[:, :part], got[:, part:]))
    (ar, ai), (br, bi), (cr, ci), (dr, di) = pieces
    er, ei, fr, fi = ar + cr, ai + ci, ar - cr, ai - ci
    gr, gi, hr, hi_ = br + dr, bi + di, br - dr, bi - di
    reals = jnp.concatenate([er + gr, fr + hi_, er - gr, fr - hi_], 1)
    imags = jnp.concatenate([ei + gi, fi - hr, ei - gi, fi + hr], 1)
    out_ref[layer, rows, 0, :] = reals.astype(jnp.bfloat16)
    out_ref[layer, rows, 1, :] = imags.astype(jnp.bfloat16)


def column_kernel(dims, *refs):
    sources = refs[:14]
    gather_ref, cos_ref, sin_ref, near_ref, fwd_ref, done_ref = refs[14:20]
    (
        shift_ref,
        offset_ref,
        start_ref,
        extent_ref,
        slot_ref,
        level_ref,
        sig_ref,
        shade_ref,
        first_ref,
        twiddle_ref,
        second_ref,
        back_ref,
        phase_ref,
    ) = refs[20:33]
    weights, mid, spec, turn, outgoing, incoming, wide, held, keeper = refs[33:42]
    pack_send, pack_recv, plane_send, block_recv, load_sem = refs[42:]
    loads = [
        pltpu.make_async_copy(source, target, load_sem.at[n])
        for n, (source, target) in enumerate(zip(sources, refs[20:33]))
    ]
    loads.append(pltpu.make_async_copy(sources[13].at[lax.axis_index("facet")], near_ref, load_sem.at[13]))
    order = [6, 7, 8, 9, 10, 0, 1, 2, 3, 4, 5, 11, 12, 13]
    for n in order:
        loads[n].start()
    facets, owners, teams, strip_rows, facet_len, grid_size, slots, total_subs = dims
    facet_id = lax.axis_index("facet")
    sub_id = lax.axis_index("sub")
    team_id = lax.axis_index("wa")
    group = facets // slots
    chunk = strip_rows // group
    width = grid_size // 2
    part = grid_size // RADIX
    cores = 2
    spread = teams // cores
    core_id = lax.rem(team_id, cores)
    sibling = team_id + 1 - 2 * core_id

    def team_at(step):
        return lax.rem(team_id + cores * step, teams)

    barrier = pltpu.get_barrier_semaphore()
    peers = 0
    for off in range(facets):
        for turn_o in range(owners):
            if off or turn_o:
                pl.semaphore_signal(
                    barrier,
                    inc=1,
                    device_id=(lax.rem(facet_id + off, facets), lax.rem(sub_id + turn_o, owners), team_id),
                    device_id_type=MESH,
                )
                peers += 1
    for step in range(1, spread):
        pl.semaphore_signal(
            barrier, inc=1, device_id=(facet_id, sub_id, team_at(step)), device_id_type=MESH
        )
        peers += 1
    pl.semaphore_signal(barrier, inc=1, device_id=(facet_id, sub_id, sibling), device_id_type=MESH)
    peers += 1

    def look(j, slot, found):
        return jnp.where(slot_ref[j] == slot, j, found)

    def holder(slot):
        if total_subs > 8:
            return lax.fori_loop(0, total_subs, lambda j, found: look(j, slot, found), jnp.int32(0))
        found = jnp.int32(0)
        for j in range(total_subs):
            found = look(j, slot, found)
        return found

    outer_len = facet_len // LANES
    fold = LANES // outer_len
    for n in order[:5]:
        loads[n].wait()
    tw_cos = twiddle_ref[0]
    tw_sin = twiddle_ref[1]

    for c in range(2):
        weights[pl.ds(c, outer_len, stride=2), :] = shade_ref[...]

    def first_step(r):
        signal = sig_ref[r].reshape(2 * outer_len, LANES).astype(jnp.float32) * weights[...]
        got = jnp.dot(first_ref[...], signal.astype(jnp.bfloat16), preferred_element_type=jnp.float32)
        real, imag = got[:outer_len], got[outer_len:]
        rows = slice(r * outer_len, (r + 1) * outer_len)
        mid[rows, :LANES] = (real * tw_cos - imag * tw_sin).astype(jnp.bfloat16)
        mid[rows, LANES:] = (real * tw_sin + imag * tw_cos).astype(jnp.bfloat16)

    for r in range(strip_rows):
        first_step(r)
    tall = LANES // fold
    lane = lax.broadcasted_iota(jnp.int32, (tall, LANES), 1)

    def second_step(i):
        rows = slice(i * LANES, (i + 1) * LANES)
        got = lax.dot_general(
            second_ref[...], mid[rows, :], (((1,), (1,)), ((), ())), preferred_element_type=jnp.float32
        )
        for c in range(2):
            even = got[c * LANES : c * LANES + tall]
            odd = got[c * LANES + tall : (c + 1) * LANES]
            near = jnp.where(lane < outer_len, even, pltpu.roll(odd, outer_len, 1))
            far = jnp.where(lane < outer_len, pltpu.roll(even, outer_len, 1), odd)
            spec[c * tall : (c + 1) * tall, i * fold, :] = near
            spec[c * tall : (c + 1) * tall, i * fold + 1, :] = far

    for i in range(strip_rows // fold):
        second_step(i)

    for n in range(6):
        loads[n].wait()
    holders = [holder(p) for p in range(total_subs)]
    for p in range(total_subs):
        keeper[p] = holders[p]
    row_ids = lax.broadcasted_iota(jnp.int32, (total_subs, width), 0)
    k_ids = lax.broadcasted_iota(jnp.int32, (total_subs, width), 1)
    starts = jnp.zeros((total_subs, width), jnp.int32)
    extents = jnp.zeros((total_subs, width), jnp.int32)
    for p in range(total_subs):
        starts = jnp.where(row_ids == p, start_ref[facet_id, holders[p]], starts)
        extents = jnp.where(row_ids == p, extent_ref[facet_id, holders[p]], extents)
    product = (shift_ref[facet_id] * (starts + k_ids)) & (grid_size - 1)
    turn_cos, turn_sin = sincos(product.astype(jnp.float32) * (2.0 * math.pi / grid_size))
    inside = k_ids < extents
    turn_cos = jnp.where(inside, turn_cos, 0.0)
    turn_sin = jnp.where(inside, turn_sin, 0.0)
    for p in range(total_subs):
        turn[0, p] = turn_cos[p : p + 1]
        turn[1, p] = turn_sin[p : p + 1]

    pl.semaphore_wait(barrier, peers)

    wide_lane = lax.broadcasted_iota(jnp.int32, (strip_rows, LANES), 1)
    pieces = width // LANES
    my_slot = facet_id // group
    packs = []
    steps = [s for s in range(slots // 2, slots)] + [s for s in range(slots // 2)][::-1]
    for turn_o in range(owners):
        for step in steps:
            slot = lax.rem(my_slot + step, slots)
            owner = lax.rem(sub_id + turn_o, owners)
            p = owner * slots + slot
            j = keeper[p]
            begin = lax.rem(offset_ref[j] + start_ref[facet_id, j], facet_len)
            q0 = lax.div(begin, LANES)
            shift = begin - q0 * LANES
            back_by = lax.rem(LANES - shift, LANES)
            tiles = []
            for c in range(2):
                rolled = []
                for q in range(pieces + 1):
                    tile = spec[c * tall + lax.rem(q0 + q, tall)]
                    rolled.append(pltpu.roll(tile, back_by, 1))
                tiles.append(
                    [jnp.where(wide_lane < LANES - shift, rolled[q], rolled[q + 1]) for q in range(pieces)]
                )
            reals, imags = [], []
            for q in range(pieces):
                lanes = slice(q * LANES, (q + 1) * LANES)
                cos = turn[0, p, :, lanes]
                sin = turn[1, p, :, lanes]
                reals.append(tiles[0][q] * cos - tiles[1][q] * sin)
                imags.append(tiles[0][q] * sin + tiles[1][q] * cos)
            block = jnp.concatenate(reals + imags, 1).astype(jnp.bfloat16)
            for g in range(group):
                target = slot * group + g
                piece = block[g * chunk : (g + 1) * chunk]
                n = len(packs)
                outgoing[n] = piece
                here = group == 1 and step == 0 and turn_o == 0
                if here:
                    incoming[facet_id, sub_id] = piece
                    packs.append((None, None))
                    continue
                copy = pltpu.make_async_remote_copy(
                    src_ref=outgoing.at[n],
                    dst_ref=incoming.at[facet_id, sub_id],
                    send_sem=pack_send.at[n],
                    recv_sem=pack_recv.at[facet_id, sub_id],
                    device_id=(target, owner, team_id),
                    device_id_type=MESH,
                )
                if step == 0 and turn_o == 0:
                    away = target != facet_id
                    pl.when(away)(copy.start)

                    @pl.when(target == facet_id)
                    def _():
                        incoming[facet_id, sub_id] = piece

                    packs.append((copy, away))
                else:
                    copy.start()
                    packs.append((copy, True))

    loads[11].wait()
    loads[12].wait()
    for p in range(RADIX):
        wide[p, :part] = back_ref[p]
        wide[p, part:, :part] = -back_ref[p][:, part:]
        wide[p, part:, part:] = back_ref[p][:, :part]
        fwd_ref[p] = wide[p].T
    mine = keeper[sub_id * slots + my_slot]
    f_rows = lax.broadcasted_iota(jnp.int32, (facets, grid_size), 0)
    at = lax.broadcasted_iota(jnp.int32, (facets, grid_size), 1)
    v_ids = (at % part) * RADIX + at // part
    begins = jnp.zeros((facets, grid_size), jnp.int32)
    for f in range(facets):
        begins = jnp.where(f_rows == f, start_ref[f, mine], begins)
    ramp_cos, ramp_sin = sincos(
        ((begins * v_ids) & (grid_size - 1)).astype(jnp.float32) * (2.0 * math.pi / grid_size)
    )
    strip_total = strip_rows * owners * teams
    scale_col = 1.0 / math.sqrt(facets * grid_size) / math.sqrt(strip_total) / math.sqrt(grid_size)
    ramp_cos = ramp_cos * scale_col
    ramp_sin = ramp_sin * scale_col

    band = phase_ref.shape[0]
    block_v = LANES * RADIX
    from_ids = lax.broadcasted_iota(jnp.int32, (block_v, block_v), 0)
    to_ids = lax.broadcasted_iota(jnp.int32, (block_v, block_v), 1)
    chosen = (from_ids == (to_ids % LANES) * RADIX + to_ids // LANES).astype(jnp.float32).astype(jnp.bfloat16)
    for h in range(grid_size // block_v):
        whole = phase_ref[:, h * block_v : (h + 1) * block_v]
        ordered = jnp.zeros((band, block_v), jnp.float32)
        for level in range(3):
            digit = whole.astype(jnp.bfloat16)
            whole = whole - digit.astype(jnp.float32)
            ordered = ordered + jnp.dot(digit, chosen, preferred_element_type=jnp.float32)
        for p in range(RADIX):
            lanes = slice(p * part + h * LANES, p * part + (h + 1) * LANES)
            for l in range(cos_ref.shape[0]):
                level_value = level_ref[team_id * cos_ref.shape[0] + l].astype(jnp.float32)
                cos, sin = sincos(level_value * ordered[:, p * LANES : (p + 1) * LANES])
                cos_ref[l, :, lanes] = cos
                sin_ref[l, :, lanes] = sin

    staged = PARTS == 2 * owners and group == 1

    def received(turn_o):
        for off in range(facets):
            if off or turn_o:
                f = lax.rem(facet_id + off, facets)
                o = lax.rem(sub_id + turn_o, owners)
                pltpu.make_async_remote_copy(
                    src_ref=incoming.at[f, o],
                    dst_ref=incoming.at[f, o],
                    send_sem=pack_send.at[0],
                    recv_sem=pack_recv.at[f, o],
                    device_id=(f, o, team_id),
                    device_id_type=MESH,
                ).wait_recv()

    def imaged(got, rows_f):
        got = got.astype(jnp.float32)
        low_r, high_r = got[:, :part], got[:, part:width]
        low_i, high_i = got[:, width : width + part], got[:, width + part :]
        images = [[], []]
        for p in range(RADIX):
            real, imag = [
                (low_r + high_r, low_i + high_i),
                (low_r - high_i, low_i + high_r),
                (low_r - high_r, low_i - high_i),
                (low_r + high_i, low_i - high_r),
            ][p]
            pair = jnp.concatenate([real.astype(jnp.bfloat16), imag.astype(jnp.bfloat16)], 1)
            moved = jnp.dot(pair, wide[p], preferred_element_type=jnp.float32)
            total_r = jnp.zeros((rows_f, part), jnp.float32)
            total_i = jnp.zeros((rows_f, part), jnp.float32)
            for f in range(facets):
                cos = ramp_cos[f : f + 1, p * part : (p + 1) * part]
                sin = ramp_sin[f : f + 1, p * part : (p + 1) * part]
                real = moved[f * rows_f : (f + 1) * rows_f, :part]
                imag = moved[f * rows_f : (f + 1) * rows_f, part:]
                total_r = total_r + (real * cos - imag * sin)
                total_i = total_i + (real * sin + imag * cos)
            images[0].append(total_r)
            images[1].append(total_i)
        return [jnp.concatenate(images[c], 1).astype(jnp.bfloat16) for c in range(2)]

    def make_part(stage):
        if staged:
            received(stage)
            o = lax.rem(sub_id + stage, owners)
            got = jnp.concatenate([incoming[f, o] for f in range(facets)], 0)
            images = imaged(got, chunk)
            for c in range(2):
                gather_ref[facet_id, team_id, c * owners + o] = images[c]
        else:
            for turn_o in range(owners):
                received(turn_o)
            got = incoming[...].reshape(facets * owners * chunk, 2 * width)
            image = jnp.concatenate(imaged(got, owners * chunk), 0)
            piece_rows = 2 * owners * chunk // PARTS
            for h in range(PARTS):
                gather_ref[facet_id, team_id, h] = image[h * piece_rows : (h + 1) * piece_rows]

    def part_at(i):
        if staged:
            return lax.rem(i, 2) * owners + lax.rem(sub_id + lax.div(i, 2), owners)
        return i

    def send(kind, f, team, h, target):
        return pltpu.make_async_remote_copy(
            src_ref=gather_ref.at[f, team, h],
            dst_ref=gather_ref.at[f, team, h],
            send_sem=plane_send.at[kind, f, team // cores, h],
            recv_sem=block_recv.at[f, team, h],
            device_id=target,
            device_id_type=MESH,
        )

    def start(copy):
        copy.start()

    def finish_send(copy):
        copy.wait_send()

    def arrive(f, team, h):
        send(0, f, team, h, (facet_id, sub_id, team_id)).wait_recv()

    below = jnp.maximum(facet_id - 1, 0)
    above = jnp.minimum(facet_id + 1, facets - 1)

    def upward(f, h, act):
        @pl.when(facet_id < facets - 1)
        def _():
            act(send(0, f, team_id, h, (above, sub_id, team_id)))

    def downward(f, h, act):
        @pl.when(facet_id > 0)
        def _():
            act(send(1, f, team_id, h, (below, sub_id, team_id)))

    def across(f, h, act):
        for step in range(1, spread):
            act(send(1 + step, f, team_id, h, (facet_id, sub_id, team_at(step))))

    def aside(f, team, h, act):
        act(send(1 + spread, f, team, h, (facet_id, sub_id, sibling)))

    def from_below(d, h):
        @pl.when(facet_id >= d)
        def _():
            f = jnp.maximum(facet_id - d, 0)
            arrive(f, team_id, h)
            upward(f, h, start)
            across(f, h, start)
            aside(f, team_id, h, start)

    def from_above(d, h):
        @pl.when(facet_id < facets - d)
        def _():
            f = jnp.minimum(facet_id + d, facets - 1)
            arrive(f, team_id, h)
            downward(f, h, start)
            aside(f, team_id, h, start)
            if d > 1:
                across(f, h, start)
            else:
                pl.when(facet_id == 0)(lambda: across(f, h, start))

    def late_across(h):
        @pl.when((facet_id > 0) & (facet_id < facets - 1))
        def _():
            across(above, h, start)

    def partner(f, h):
        for step in range(1, spread):
            arrive(f, team_at(step), h)
            aside(f, team_at(step), h, start)

    def settled(f, h):
        for step in range(spread):
            arrive(f, lax.rem(sibling + cores * step, teams), h)

    def each_part(body, first=0, last=PARTS):
        def run(i, carry):
            body(part_at(i))
            return carry

        lax.fori_loop(first, last, run, 0)

    sequence = arrivals(facets, facet_id)
    early = facets - 1 if done_ref.shape[2] == cos_ref.shape[1] else 0

    def own(h):
        upward(facet_id, h, start)
        downward(facet_id, h, start)
        across(facet_id, h, start)
        aside(facet_id, team_id, h, start)

    def neighbours(h):
        from_below(1, h)
        from_above(1, h)
        partner(facet_id, h)

    stages = owners if staged else 1
    for stage in range(stages):
        make_part(stage)
        if stage == 0:
            loads[13].wait()
        span = PARTS // stages
        each_part(own, stage * span, (stage + 1) * span)
        each_part(neighbours, stage * span, (stage + 1) * span)
    each_part(late_across)
    each_part(lambda h: settled(sequence[0], h))
    for k in range(facets - 1):

        def relay(i, carry, k=k):
            h = part_at(i)
            if k + 2 < facets:
                from_below(k + 2, h)
                from_above(k + 2, h)
            partner(sequence[k + 1], h)
            if k < early:
                unit(i, gather_ref, sequence[k], near_ref, fwd_ref, cos_ref, sin_ref, held, done_ref.at[k])
            return carry

        lax.fori_loop(0, PARTS, relay, 0)
        each_part(lambda h, k=k: settled(sequence[k + 1], h))

    def drain(h):
        upward(facet_id, h, finish_send)
        downward(facet_id, h, finish_send)
        across(facet_id, h, finish_send)
        aside(facet_id, team_id, h, finish_send)
        for step in range(1, spread):
            aside(facet_id, team_at(step), h, finish_send)
        for d in range(1, facets):

            @pl.when(facet_id >= d)
            def _(d=d):
                f = jnp.maximum(facet_id - d, 0)
                upward(f, h, finish_send)
                across(f, h, finish_send)
                aside(f, team_id, h, finish_send)
                for step in range(1, spread):
                    aside(f, team_at(step), h, finish_send)

            @pl.when(facet_id < facets - d)
            def _(d=d):
                f = jnp.minimum(facet_id + d, facets - 1)
                downward(f, h, finish_send)
                across(f, h, finish_send)
                aside(f, team_id, h, finish_send)
                for step in range(1, spread):
                    aside(f, team_at(step), h, finish_send)

    each_part(drain)
    for copy, away in packs:
        if away is True:
            copy.wait_send()
        elif away is not None:
            pl.when(away)(copy.wait_send)


def column(scalars, sig, shade, tables, left, phase, dims, layers, early):
    facets, owners, teams, strip_rows, facet_len, grid_size, slots, total_subs = dims
    first, twiddle, second, back = [jnp.asarray(x) for x in tables]
    group = facets // slots
    chunk = strip_rows // group
    width = grid_size // 2
    part = grid_size // RADIX
    band = phase.shape[0]
    hbm = pl.BlockSpec(memory_space=pltpu.HBM)
    vmem = pl.BlockSpec(memory_space=pltpu.VMEM)
    operands = [*scalars, sig, shade, first, twiddle, second, back, phase]
    blocks = (facets, teams, PARTS, 2 * owners * chunk // PARTS, grid_size)
    spread = teams // 2
    return pl.pallas_call(
        functools.partial(column_kernel, dims),
        out_shape=[
            jax.ShapeDtypeStruct(blocks, jnp.bfloat16),
            jax.ShapeDtypeStruct((layers, band, grid_size), jnp.float32),
            jax.ShapeDtypeStruct((layers, band, grid_size), jnp.float32),
            jax.ShapeDtypeStruct(left.shape[1:], jnp.bfloat16),
            jax.ShapeDtypeStruct((RADIX, 2 * part, 2 * part), jnp.bfloat16),
            jax.ShapeDtypeStruct((max(early, 1), layers, band if early else 16, 2, grid_size), jnp.bfloat16),
        ],
        in_specs=[hbm] * 14,
        out_specs=[vmem] * 6,
        scratch_shapes=[pltpu.SMEM(x.shape, x.dtype) for x in operands[:6]]
        + [pltpu.VMEM(x.shape, x.dtype) for x in operands[6:]]
        + [
            pltpu.VMEM((2 * facet_len // LANES, LANES), jnp.float32),
            pltpu.VMEM((strip_rows * (facet_len // LANES), 2 * LANES), jnp.bfloat16),
            pltpu.VMEM((2 * facet_len // LANES, strip_rows, LANES), jnp.float32),
            pltpu.VMEM((2, total_subs, 1, width), jnp.float32),
            pltpu.VMEM((facets * owners, chunk, 2 * width), jnp.bfloat16),
            pltpu.VMEM((facets, owners, chunk, 2 * width), jnp.bfloat16),
            pltpu.VMEM((RADIX, 2 * part, 2 * part), jnp.bfloat16),
            pltpu.VMEM((2 * band // HALVES, grid_size), jnp.bfloat16),
            pltpu.SMEM((total_subs,), jnp.int32),
            pltpu.SemaphoreType.DMA((facets * owners,)),
            pltpu.SemaphoreType.DMA((facets, owners)),
            pltpu.SemaphoreType.DMA((2 + spread, facets, spread, PARTS)),
            pltpu.SemaphoreType.DMA((facets, teams, PARTS)),
            pltpu.SemaphoreType.DMA((14,)),
        ],
        compiler_params=pltpu.CompilerParams(
            collective_id=0, has_side_effects=True, vmem_limit_bytes=VMEM_COLUMN
        ),
        cost_estimate=pl.CostEstimate(flops=2_000_000_000, bytes_accessed=20_000_000, transcendentals=0),
    )(*[pltpu.with_memory_space_constraint(x, pltpu.HBM) for x in operands + [left]])


def finish_kernel(early, facets, right_ref, cos_ref, sin_ref, near_ref, fwd_ref, done_ref, out_ref, held, ready, done_sem, ready_sem):
    layers, band, grid_size = cos_ref.shape
    slots = out_ref.shape[0]
    half = band // HALVES
    if early:
        sequence = arrivals(facets, lax.axis_index("facet"))
    else:
        sequence = list(range(slots))
    moved = []
    for k in range(early):
        moved.append(pltpu.make_async_copy(done_ref.at[k], out_ref.at[sequence[k]], done_sem.at[k]))
        moved[-1].start()

    def ship(slot, step):
        layer = lax.rem(step, layers)
        rows = pl.ds(pl.multiple_of(lax.div(step, layers) * half, half), half)
        return pltpu.make_async_copy(
            ready.at[layer, rows], out_ref.at[slot, layer, rows], ready_sem.at[step]
        )

    for k in range(early, slots):

        def run(step, carry, k=k):
            if k > early:
                ship(sequence[k - 1], step).wait()
            unit(step, right_ref, sequence[k], near_ref, fwd_ref, cos_ref, sin_ref, held, ready)
            ship(sequence[k], step).start()
            return carry

        lax.fori_loop(0, layers * HALVES, run, 0)
    for step in range(layers * HALVES):
        ship(sequence[slots - 1], step).wait()
    for copy in moved:
        copy.wait()


def finish(right, cos, sin, near, fwd, done, early, facets):
    layers, band, grid_size = cos.shape
    slots = right.shape[0]
    vmem = pl.BlockSpec(memory_space=pltpu.VMEM)
    return pl.pallas_call(
        functools.partial(finish_kernel, early, facets),
        out_shape=jax.ShapeDtypeStruct((slots, layers, band, 2, grid_size), jnp.bfloat16),
        in_specs=[vmem] * 6,
        out_specs=pl.BlockSpec(memory_space=pl.ANY),
        scratch_shapes=[
            pltpu.VMEM((2 * band // HALVES, grid_size), jnp.bfloat16),
            pltpu.VMEM((layers, band, 2, grid_size), jnp.bfloat16),
            pltpu.SemaphoreType.DMA((max(early, 1),)),
            pltpu.SemaphoreType.DMA((layers * HALVES,)),
        ],
        compiler_params=pltpu.CompilerParams(vmem_limit_bytes=VMEM_FINISH),
        cost_estimate=pl.CostEstimate(flops=2_000_000_000, bytes_accessed=20_000_000, transcendentals=0),
    )(right, cos, sin, near, fwd, done)


def local(
    facet_data,
    window,
    screen_phase,
    facet_shift,
    sub_offset,
    win_start,
    win_extent,
    owner_slot,
    layer_w,
):
    facets = lax.axis_size("facet")
    owners = lax.axis_size("sub")
    teams = lax.axis_size("wa")
    strip_rows = facet_data.shape[1]
    facet_len = facet_data.shape[3]
    band, grid_size = screen_phase.shape
    total_subs = owner_slot.shape[0]
    slots = total_subs // owners
    group = facets // slots
    chunk = strip_rows // group
    strip_total = strip_rows * owners * teams
    layers = layer_w.shape[0] // teams
    dims = (facets, owners, teams, strip_rows, facet_len, grid_size, slots, total_subs)

    outer_len = facet_len // LANES
    sig = facet_data[0].reshape(strip_rows, 2, outer_len, LANES).transpose(0, 2, 1, 3)
    shade = window.reshape(outer_len, LANES)
    tables = strip_tables(facet_len, grid_size)
    scalars = (facet_shift, sub_offset, win_start, win_extent, owner_slot, layer_w)
    g_ids, t_ids, c_ids, o_ids, r_ids = np.meshgrid(
        np.arange(group), np.arange(teams), np.arange(2), np.arange(owners), np.arange(chunk), indexing="ij"
    )
    global_row = ((o_ids * teams + t_ids) * strip_rows + g_ids * chunk + r_ids).reshape(1, 1, -1)
    is_imag = c_ids.reshape(1, 1, -1)
    my_rows = np.arange(grid_size).reshape(facets * HALVES, band // HALVES, 1)
    all_cos, all_sin = table(my_rows * global_row, grid_size, -1.0)
    real_rows = np.where(is_imag == 1, -all_sin, all_cos)
    imag_rows = np.where(is_imag == 1, all_cos, all_sin)
    left = np.concatenate([real_rows, imag_rows], 1).astype(jnp.bfloat16)
    left = jnp.asarray(left.reshape(facets, HALVES, 2 * band // HALVES, 2 * strip_total))

    early = facets - 1 if group == 1 and layers * HALVES == PARTS else 0
    right, cos, sin, near, fwd, done = column(scalars, sig, shade, tables, left, screen_phase, dims, layers, early)
    if not early:
        right = right.reshape(slots, 2 * strip_total, grid_size)
    return finish(right, cos, sin, near, fwd, done, early, facets)


def solution(mesh):
    in_specs = (
        P("facet", ("sub", "wa"), None, None),
        P(),
        P("facet", None),
        P(),
        P(),
        P(),
        P(),
        P(),
        P(),
    )
    out_specs = P("sub", "wa", "facet", None, None)
    return jax.shard_map(local, mesh=mesh, in_specs=in_specs, out_specs=out_specs, check_vma=False)
```

```python
import functools
import math

import jax
import jax.numpy as jnp
import numpy as np
from jax import lax
from jax.experimental import pallas as pl
from jax.experimental.pallas import tpu as pltpu
from jax.sharding import PartitionSpec as P

RADIX = 4
LANES = 128
PARTS = 4
HALVES = 2
VMEM_COLUMN = 32 * 1024 * 1024
VMEM_FINISH = 32 * 1024 * 1024
MESH = pl.DeviceIdType.MESH


def table(products, modulus, sign_value):
    angles = (sign_value * 2.0 * math.pi / modulus) * (products % modulus).astype(np.float64)
    return np.cos(angles), np.sin(angles)


def sincos(angles):
    turns = jnp.floor(angles * (2.0 / math.pi) + 0.5)
    rest = angles - turns * 1.5703125
    rest = rest - turns * 4.837512969970703e-4
    rest = rest - turns * 7.549789948768648e-8
    square = rest * rest
    sine = rest + rest * square * (
        -1.6666654611e-1 + square * (8.3321608736e-3 + square * -1.9515295891e-4)
    )
    cosine = (1.0 - 0.5 * square) + square * square * (
        4.166664568298827e-2 + square * (-1.388731625493765e-3 + square * 2.443315711809948e-5)
    )
    quadrant = turns.astype(jnp.int32)
    odd = (quadrant & 1) == 1
    sin_size = jnp.where(odd, cosine, sine)
    cos_size = jnp.where(odd, sine, cosine)
    sin_value = jnp.where((quadrant & 2) == 2, -sin_size, sin_size)
    cos_value = jnp.where(((quadrant + 1) & 2) == 2, -cos_size, cos_size)
    return cos_value, sin_value


def strip_tables(facet_len, grid_size):
    inner_len = LANES
    outer_len = facet_len // inner_len
    outer_ids = np.arange(outer_len)
    inner_ids = np.arange(inner_len)
    c1, s1 = table(outer_ids[:, None] * outer_ids[None, :], outer_len, -1.0)
    first = np.block([[c1, -s1], [s1, c1]])
    first = first.reshape(-1, 2, outer_len).transpose(0, 2, 1).reshape(-1, 2 * outer_len).astype(jnp.bfloat16)
    ct, st = table(outer_ids[:, None] * inner_ids[None, :], facet_len, -1.0)
    twiddle = np.stack([ct, st]).astype(np.float32)
    fold = LANES // outer_len
    q_ids = (np.arange(inner_len // fold)[None, :] * fold + np.arange(fold)[:, None]).reshape(-1)
    c2, s2 = table(q_ids[:, None] * inner_ids[None, :], inner_len, -1.0)
    scale = 1.0 / math.sqrt(facet_len)
    second = (np.block([[c2, -s2], [s2, c2]]) * scale).astype(jnp.bfloat16)
    part = grid_size // RADIX
    v_ids = np.arange(part)[None, :] * RADIX + np.arange(RADIX)[:, None]
    bc, bs = table(np.arange(part)[None, :, None] * v_ids[:, None, :], grid_size, 1.0)
    back = np.concatenate([bc, bs], 2).astype(jnp.bfloat16)
    return first, twiddle, second, back


def arrivals(facets, facet_id):
    order = []
    for z in range(facets):
        row = [z]
        for d in range(1, facets):
            row += [f for f in (z - d, z + d) if 0 <= f < facets]
        order.append(row)
    picked = []
    for k in range(facets):
        value = 0
        for z in range(facets):
            gap = facet_id - z
            here = 1 - lax.div(gap * gap + (facets * facets - 1), facets * facets)
            value = value + here * order[z][k]
        picked.append(value)
    return picked


def unit(step, right_ref, slot, near_ref, fwd_ref, cos_ref, sin_ref, held, out_ref):
    layers, band, grid_size = cos_ref.shape
    part = grid_size // RADIX
    half = band // HALVES
    layer = lax.rem(step, layers)
    which = lax.div(step, layers)
    rows = pl.ds(pl.multiple_of(which * half, half), half)

    @pl.when(layer == 0)
    def _():
        right = right_ref[slot].reshape(near_ref.shape[2], grid_size)
        for p in range(RADIX):
            lanes = slice(p * part, (p + 1) * part)
            got = jnp.dot(near_ref[which], right[:, lanes], preferred_element_type=jnp.float32)
            held[:, lanes] = got.astype(jnp.bfloat16)

    pieces = []
    for p in range(RADIX):
        lanes = slice(p * part, (p + 1) * part)
        real = held[:half, lanes].astype(jnp.float32)
        imag = held[half:, lanes].astype(jnp.float32)
        cos = cos_ref[layer, rows, lanes]
        sin = sin_ref[layer, rows, lanes]
        s_real = (real * cos - imag * sin).astype(jnp.bfloat16)
        s_imag = (real * sin + imag * cos).astype(jnp.bfloat16)
        pair = jnp.concatenate([s_real, s_imag], 1)
        got = jnp.dot(pair, fwd_ref[p], preferred_element_type=jnp.float32)
        pieces.append((got[:, :part], got[:, part:]))
    (ar, ai), (br, bi), (cr, ci), (dr, di) = pieces
    er, ei, fr, fi = ar + cr, ai + ci, ar - cr, ai - ci
    gr, gi, hr, hi_ = br + dr, bi + di, br - dr, bi - di
    reals = jnp.concatenate([er + gr, fr + hi_, er - gr, fr - hi_], 1)
    imags = jnp.concatenate([ei + gi, fi - hr, ei - gi, fi + hr], 1)
    out_ref[layer, rows, 0, :] = reals.astype(jnp.bfloat16)
    out_ref[layer, rows, 1, :] = imags.astype(jnp.bfloat16)


def column_kernel(dims, *refs):
    sources = refs[:14]
    gather_ref, cos_ref, sin_ref, near_ref, fwd_ref, done_ref = refs[14:20]
    (
        shift_ref,
        offset_ref,
        start_ref,
        extent_ref,
        slot_ref,
        level_ref,
        sig_ref,
        shade_ref,
        first_ref,
        twiddle_ref,
        second_ref,
        back_ref,
        phase_ref,
    ) = refs[20:33]
    weights, mid, spec, turn, outgoing, incoming, wide, held, keeper = refs[33:42]
    pack_send, pack_recv, plane_send, block_recv, load_sem = refs[42:]
    loads = [
        pltpu.make_async_copy(source, target, load_sem.at[n])
        for n, (source, target) in enumerate(zip(sources, refs[20:33]))
    ]
    loads.append(pltpu.make_async_copy(sources[13].at[lax.axis_index("facet")], near_ref, load_sem.at[13]))
    order = [6, 7, 8, 9, 10, 0, 1, 2, 3, 4, 5, 11, 12, 13]
    for n in order:
        loads[n].start()
    facets, owners, teams, strip_rows, facet_len, grid_size, slots, total_subs = dims
    facet_id = lax.axis_index("facet")
    sub_id = lax.axis_index("sub")
    team_id = lax.axis_index("wa")
    group = facets // slots
    chunk = strip_rows // group
    width = grid_size // 2
    part = grid_size // RADIX
    cores = 2
    spread = teams // cores
    core_id = lax.rem(team_id, cores)
    sibling = team_id + 1 - 2 * core_id

    def team_at(step):
        return lax.rem(team_id + cores * step, teams)

    barrier = pltpu.get_barrier_semaphore()
    peers = 0
    for off in range(facets):
        for turn_o in range(owners):
            if off or turn_o:
                pl.semaphore_signal(
                    barrier,
                    inc=1,
                    device_id=(lax.rem(facet_id + off, facets), lax.rem(sub_id + turn_o, owners), team_id),
                    device_id_type=MESH,
                )
                peers += 1
    for step in range(1, spread):
        pl.semaphore_signal(
            barrier, inc=1, device_id=(facet_id, sub_id, team_at(step)), device_id_type=MESH
        )
        peers += 1
    pl.semaphore_signal(barrier, inc=1, device_id=(facet_id, sub_id, sibling), device_id_type=MESH)
    peers += 1

    def look(j, slot, found):
        return jnp.where(slot_ref[j] == slot, j, found)

    def holder(slot):
        if total_subs > 8:
            return lax.fori_loop(0, total_subs, lambda j, found: look(j, slot, found), jnp.int32(0))
        found = jnp.int32(0)
        for j in range(total_subs):
            found = look(j, slot, found)
        return found

    outer_len = facet_len // LANES
    fold = LANES // outer_len
    for n in order[:5]:
        loads[n].wait()
    tw_cos = twiddle_ref[0]
    tw_sin = twiddle_ref[1]

    for c in range(2):
        weights[pl.ds(c, outer_len, stride=2), :] = shade_ref[...]

    def first_step(r):
        signal = sig_ref[r].reshape(2 * outer_len, LANES).astype(jnp.float32) * weights[...]
        got = jnp.dot(first_ref[...], signal.astype(jnp.bfloat16), preferred_element_type=jnp.float32)
        real, imag = got[:outer_len], got[outer_len:]
        rows = slice(r * outer_len, (r + 1) * outer_len)
        mid[rows, :LANES] = (real * tw_cos - imag * tw_sin).astype(jnp.bfloat16)
        mid[rows, LANES:] = (real * tw_sin + imag * tw_cos).astype(jnp.bfloat16)

    for r in range(strip_rows):
        first_step(r)
    tall = LANES // fold
    lane = lax.broadcasted_iota(jnp.int32, (tall, LANES), 1)

    def second_step(i):
        rows = slice(i * LANES, (i + 1) * LANES)
        got = lax.dot_general(
            second_ref[...], mid[rows, :], (((1,), (1,)), ((), ())), preferred_element_type=jnp.float32
        )
        for c in range(2):
            even = got[c * LANES : c * LANES + tall]
            odd = got[c * LANES + tall : (c + 1) * LANES]
            near = jnp.where(lane < outer_len, even, pltpu.roll(odd, outer_len, 1))
            far = jnp.where(lane < outer_len, pltpu.roll(even, outer_len, 1), odd)
            spec[c * tall : (c + 1) * tall, i * fold, :] = near
            spec[c * tall : (c + 1) * tall, i * fold + 1, :] = far

    for i in range(strip_rows // fold):
        second_step(i)

    for n in range(6):
        loads[n].wait()
    holders = [holder(p) for p in range(total_subs)]
    for p in range(total_subs):
        keeper[p] = holders[p]
    row_ids = lax.broadcasted_iota(jnp.int32, (total_subs, width), 0)
    k_ids = lax.broadcasted_iota(jnp.int32, (total_subs, width), 1)
    starts = jnp.zeros((total_subs, width), jnp.int32)
    extents = jnp.zeros((total_subs, width), jnp.int32)
    for p in range(total_subs):
        starts = jnp.where(row_ids == p, start_ref[facet_id, holders[p]], starts)
        extents = jnp.where(row_ids == p, extent_ref[facet_id, holders[p]], extents)
    product = (shift_ref[facet_id] * (starts + k_ids)) & (grid_size - 1)
    turn_cos, turn_sin = sincos(product.astype(jnp.float32) * (2.0 * math.pi / grid_size))
    inside = k_ids < extents
    turn_cos = jnp.where(inside, turn_cos, 0.0)
    turn_sin = jnp.where(inside, turn_sin, 0.0)
    for p in range(total_subs):
        turn[0, p] = turn_cos[p : p + 1]
        turn[1, p] = turn_sin[p : p + 1]

    pl.semaphore_wait(barrier, peers)

    wide_lane = lax.broadcasted_iota(jnp.int32, (strip_rows, LANES), 1)
    pieces = width // LANES
    my_slot = facet_id // group
    packs = []
    steps = [s for s in range(slots // 2, slots)] + [s for s in range(slots // 2)][::-1]
    for turn_o in range(owners):
        for step in steps:
            slot = lax.rem(my_slot + step, slots)
            owner = lax.rem(sub_id + turn_o, owners)
            p = owner * slots + slot
            j = keeper[p]
            begin = lax.rem(offset_ref[j] + start_ref[facet_id, j], facet_len)
            q0 = lax.div(begin, LANES)
            shift = begin - q0 * LANES
            back_by = lax.rem(LANES - shift, LANES)
            tiles = []
            for c in range(2):
                rolled = []
                for q in range(pieces + 1):
                    tile = spec[c * tall + lax.rem(q0 + q, tall)]
                    rolled.append(pltpu.roll(tile, back_by, 1))
                tiles.append(
                    [jnp.where(wide_lane < LANES - shift, rolled[q], rolled[q + 1]) for q in range(pieces)]
                )
            reals, imags = [], []
            for q in range(pieces):
                lanes = slice(q * LANES, (q + 1) * LANES)
                cos = turn[0, p, :, lanes]
                sin = turn[1, p, :, lanes]
                reals.append(tiles[0][q] * cos - tiles[1][q] * sin)
                imags.append(tiles[0][q] * sin + tiles[1][q] * cos)
            block = jnp.concatenate(reals + imags, 1).astype(jnp.bfloat16)
            for g in range(group):
                target = slot * group + g
                piece = block[g * chunk : (g + 1) * chunk]
                n = len(packs)
                outgoing[n] = piece
                here = group == 1 and step == 0 and turn_o == 0
                if here:
                    incoming[facet_id, sub_id] = piece
                    packs.append((None, None))
                    continue
                copy = pltpu.make_async_remote_copy(
                    src_ref=outgoing.at[n],
                    dst_ref=incoming.at[facet_id, sub_id],
                    send_sem=pack_send.at[n],
                    recv_sem=pack_recv.at[facet_id, sub_id],
                    device_id=(target, owner, team_id),
                    device_id_type=MESH,
                )
                if step == 0 and turn_o == 0:
                    away = target != facet_id
                    pl.when(away)(copy.start)

                    @pl.when(target == facet_id)
                    def _():
                        incoming[facet_id, sub_id] = piece

                    packs.append((copy, away))
                else:
                    copy.start()
                    packs.append((copy, True))

    loads[11].wait()
    loads[12].wait()
    for p in range(RADIX):
        wide[p, :part] = back_ref[p]
        wide[p, part:, :part] = -back_ref[p][:, part:]
        wide[p, part:, part:] = back_ref[p][:, :part]
        fwd_ref[p] = wide[p].T
    mine = keeper[sub_id * slots + my_slot]
    f_rows = lax.broadcasted_iota(jnp.int32, (facets, grid_size), 0)
    at = lax.broadcasted_iota(jnp.int32, (facets, grid_size), 1)
    v_ids = (at % part) * RADIX + at // part
    begins = jnp.zeros((facets, grid_size), jnp.int32)
    for f in range(facets):
        begins = jnp.where(f_rows == f, start_ref[f, mine], begins)
    ramp_cos, ramp_sin = sincos(
        ((begins * v_ids) & (grid_size - 1)).astype(jnp.float32) * (2.0 * math.pi / grid_size)
    )
    strip_total = strip_rows * owners * teams
    scale_col = 1.0 / math.sqrt(facets * grid_size) / math.sqrt(strip_total) / math.sqrt(grid_size)
    ramp_cos = ramp_cos * scale_col
    ramp_sin = ramp_sin * scale_col

    band = phase_ref.shape[0]
    block_v = LANES * RADIX
    from_ids = lax.broadcasted_iota(jnp.int32, (block_v, block_v), 0)
    to_ids = lax.broadcasted_iota(jnp.int32, (block_v, block_v), 1)
    chosen = (from_ids == (to_ids % LANES) * RADIX + to_ids // LANES).astype(jnp.float32).astype(jnp.bfloat16)
    for h in range(grid_size // block_v):
        whole = phase_ref[:, h * block_v : (h + 1) * block_v]
        ordered = jnp.zeros((band, block_v), jnp.float32)
        for level in range(3):
            digit = whole.astype(jnp.bfloat16)
            whole = whole - digit.astype(jnp.float32)
            ordered = ordered + jnp.dot(digit, chosen, preferred_element_type=jnp.float32)
        for p in range(RADIX):
            lanes = slice(p * part + h * LANES, p * part + (h + 1) * LANES)
            for l in range(cos_ref.shape[0]):
                level_value = level_ref[team_id * cos_ref.shape[0] + l].astype(jnp.float32)
                cos, sin = sincos(level_value * ordered[:, p * LANES : (p + 1) * LANES])
                cos_ref[l, :, lanes] = cos
                sin_ref[l, :, lanes] = sin

    staged = PARTS == 2 * owners and group == 1

    def received(turn_o):
        for off in range(facets):
            if off or turn_o:
                f = lax.rem(facet_id + off, facets)
                o = lax.rem(sub_id + turn_o, owners)
                pltpu.make_async_remote_copy(
                    src_ref=incoming.at[f, o],
                    dst_ref=incoming.at[f, o],
                    send_sem=pack_send.at[0],
                    recv_sem=pack_recv.at[f, o],
                    device_id=(f, o, team_id),
                    device_id_type=MESH,
                ).wait_recv()

    def imaged(got, rows_f):
        got = got.astype(jnp.float32)
        low_r, high_r = got[:, :part], got[:, part:width]
        low_i, high_i = got[:, width : width + part], got[:, width + part :]
        images = [[], []]
        for p in range(RADIX):
            real, imag = [
                (low_r + high_r, low_i + high_i),
                (low_r - high_i, low_i + high_r),
                (low_r - high_r, low_i - high_i),
                (low_r + high_i, low_i - high_r),
            ][p]
            pair = jnp.concatenate([real.astype(jnp.bfloat16), imag.astype(jnp.bfloat16)], 1)
            moved = jnp.dot(pair, wide[p], preferred_element_type=jnp.float32)
            total_r = jnp.zeros((rows_f, part), jnp.float32)
            total_i = jnp.zeros((rows_f, part), jnp.float32)
            for f in range(facets):
                cos = ramp_cos[f : f + 1, p * part : (p + 1) * part]
                sin = ramp_sin[f : f + 1, p * part : (p + 1) * part]
                real = moved[f * rows_f : (f + 1) * rows_f, :part]
                imag = moved[f * rows_f : (f + 1) * rows_f, part:]
                total_r = total_r + (real * cos - imag * sin)
                total_i = total_i + (real * sin + imag * cos)
            images[0].append(total_r)
            images[1].append(total_i)
        return [jnp.concatenate(images[c], 1).astype(jnp.bfloat16) for c in range(2)]

    def make_part(stage):
        if staged:
            received(stage)
            o = lax.rem(sub_id + stage, owners)
            got = jnp.concatenate([incoming[f, o] for f in range(facets)], 0)
            images = imaged(got, chunk)
            for c in range(2):
                gather_ref[facet_id, team_id, c * owners + o] = images[c]
        else:
            for turn_o in range(owners):
                received(turn_o)
            got = incoming[...].reshape(facets * owners * chunk, 2 * width)
            image = jnp.concatenate(imaged(got, owners * chunk), 0)
            piece_rows = 2 * owners * chunk // PARTS
            for h in range(PARTS):
                gather_ref[facet_id, team_id, h] = image[h * piece_rows : (h + 1) * piece_rows]

    def part_at(i):
        if staged:
            return lax.rem(i, 2) * owners + lax.rem(sub_id + lax.div(i, 2), owners)
        return i

    def send(kind, f, team, h, target):
        return pltpu.make_async_remote_copy(
            src_ref=gather_ref.at[f, team, h],
            dst_ref=gather_ref.at[f, team, h],
            send_sem=plane_send.at[kind, f, team // cores, h],
            recv_sem=block_recv.at[f, team, h],
            device_id=target,
            device_id_type=MESH,
        )

    def start(copy):
        copy.start()

    def finish_send(copy):
        copy.wait_send()

    def arrive(f, team, h):
        send(0, f, team, h, (facet_id, sub_id, team_id)).wait_recv()

    below = jnp.maximum(facet_id - 1, 0)
    above = jnp.minimum(facet_id + 1, facets - 1)

    def upward(f, h, act):
        @pl.when(facet_id < facets - 1)
        def _():
            act(send(0, f, team_id, h, (above, sub_id, team_id)))

    def downward(f, h, act):
        @pl.when(facet_id > 0)
        def _():
            act(send(1, f, team_id, h, (below, sub_id, team_id)))

    def across(f, h, act):
        for step in range(1, spread):
            act(send(1 + step, f, team_id, h, (facet_id, sub_id, team_at(step))))

    def aside(f, team, h, act):
        act(send(1 + spread, f, team, h, (facet_id, sub_id, sibling)))

    def from_below(d, h):
        @pl.when(facet_id >= d)
        def _():
            f = jnp.maximum(facet_id - d, 0)
            arrive(f, team_id, h)
            upward(f, h, start)
            across(f, h, start)
            aside(f, team_id, h, start)

    def from_above(d, h):
        @pl.when(facet_id < facets - d)
        def _():
            f = jnp.minimum(facet_id + d, facets - 1)
            arrive(f, team_id, h)
            downward(f, h, start)
            aside(f, team_id, h, start)
            if d > 1:
                across(f, h, start)
            else:
                pl.when(facet_id == 0)(lambda: across(f, h, start))

    def late_across(h):
        @pl.when((facet_id > 0) & (facet_id < facets - 1))
        def _():
            across(above, h, start)

    def partner(f, h):
        for step in range(1, spread):
            arrive(f, team_at(step), h)
            aside(f, team_at(step), h, start)

    def settled(f, h):
        for step in range(spread):
            arrive(f, lax.rem(sibling + cores * step, teams), h)

    def each_part(body, first=0, last=PARTS):
        def run(i, carry):
            body(part_at(i))
            return carry

        lax.fori_loop(first, last, run, 0, unroll=True)

    sequence = arrivals(facets, facet_id)
    early = facets - 1 if done_ref.shape[2] == cos_ref.shape[1] else 0

    def own(h):
        upward(facet_id, h, start)
        downward(facet_id, h, start)
        across(facet_id, h, start)
        aside(facet_id, team_id, h, start)

    def neighbours(h):
        from_below(1, h)
        from_above(1, h)
        partner(facet_id, h)

    stages = owners if staged else 1
    for stage in range(stages):
        make_part(stage)
        if stage == 0:
            loads[13].wait()
        span = PARTS // stages
        each_part(own, stage * span, (stage + 1) * span)
        each_part(neighbours, stage * span, (stage + 1) * span)
    each_part(late_across)
    each_part(lambda h: settled(sequence[0], h))
    for k in range(facets - 1):

        def relay(i, carry, k=k):
            h = part_at(i)
            if k + 2 < facets:
                from_below(k + 2, h)
                from_above(k + 2, h)
            partner(sequence[k + 1], h)
            if k < early:
                unit(i, gather_ref, sequence[k], near_ref, fwd_ref, cos_ref, sin_ref, held, done_ref.at[k])
            return carry

        lax.fori_loop(0, PARTS, relay, 0)
        each_part(lambda h, k=k: settled(sequence[k + 1], h))

    def drain(h):
        upward(facet_id, h, finish_send)
        downward(facet_id, h, finish_send)
        across(facet_id, h, finish_send)
        aside(facet_id, team_id, h, finish_send)
        for step in range(1, spread):
            aside(facet_id, team_at(step), h, finish_send)
        for d in range(1, facets):

            @pl.when(facet_id >= d)
            def _(d=d):
                f = jnp.maximum(facet_id - d, 0)
                upward(f, h, finish_send)
                across(f, h, finish_send)
                aside(f, team_id, h, finish_send)
                for step in range(1, spread):
                    aside(f, team_at(step), h, finish_send)

            @pl.when(facet_id < facets - d)
            def _(d=d):
                f = jnp.minimum(facet_id + d, facets - 1)
                downward(f, h, finish_send)
                across(f, h, finish_send)
                aside(f, team_id, h, finish_send)
                for step in range(1, spread):
                    aside(f, team_at(step), h, finish_send)

    each_part(drain)
    for copy, away in packs:
        if away is True:
            copy.wait_send()
        elif away is not None:
            pl.when(away)(copy.wait_send)


def column(scalars, sig, shade, tables, left, phase, dims, layers, early):
    facets, owners, teams, strip_rows, facet_len, grid_size, slots, total_subs = dims
    first, twiddle, second, back = [jnp.asarray(x) for x in tables]
    group = facets // slots
    chunk = strip_rows // group
    width = grid_size // 2
    part = grid_size // RADIX
    band = phase.shape[0]
    hbm = pl.BlockSpec(memory_space=pltpu.HBM)
    vmem = pl.BlockSpec(memory_space=pltpu.VMEM)
    operands = [*scalars, sig, shade, first, twiddle, second, back, phase]
    blocks = (facets, teams, PARTS, 2 * owners * chunk // PARTS, grid_size)
    spread = teams // 2
    return pl.pallas_call(
        functools.partial(column_kernel, dims),
        out_shape=[
            jax.ShapeDtypeStruct(blocks, jnp.bfloat16),
            jax.ShapeDtypeStruct((layers, band, grid_size), jnp.float32),
            jax.ShapeDtypeStruct((layers, band, grid_size), jnp.float32),
            jax.ShapeDtypeStruct(left.shape[1:], jnp.bfloat16),
            jax.ShapeDtypeStruct((RADIX, 2 * part, 2 * part), jnp.bfloat16),
            jax.ShapeDtypeStruct((max(early, 1), layers, band if early else 16, 2, grid_size), jnp.bfloat16),
        ],
        in_specs=[hbm] * 14,
        out_specs=[vmem] * 6,
        scratch_shapes=[pltpu.SMEM(x.shape, x.dtype) for x in operands[:6]]
        + [pltpu.VMEM(x.shape, x.dtype) for x in operands[6:]]
        + [
            pltpu.VMEM((2 * facet_len // LANES, LANES), jnp.float32),
            pltpu.VMEM((strip_rows * (facet_len // LANES), 2 * LANES), jnp.bfloat16),
            pltpu.VMEM((2 * facet_len // LANES, strip_rows, LANES), jnp.float32),
            pltpu.VMEM((2, total_subs, 1, width), jnp.float32),
            pltpu.VMEM((facets * owners, chunk, 2 * width), jnp.bfloat16),
            pltpu.VMEM((facets, owners, chunk, 2 * width), jnp.bfloat16),
            pltpu.VMEM((RADIX, 2 * part, 2 * part), jnp.bfloat16),
            pltpu.VMEM((2 * band // HALVES, grid_size), jnp.bfloat16),
            pltpu.SMEM((total_subs,), jnp.int32),
            pltpu.SemaphoreType.DMA((facets * owners,)),
            pltpu.SemaphoreType.DMA((facets, owners)),
            pltpu.SemaphoreType.DMA((2 + spread, facets, spread, PARTS)),
            pltpu.SemaphoreType.DMA((facets, teams, PARTS)),
            pltpu.SemaphoreType.DMA((14,)),
        ],
        compiler_params=pltpu.CompilerParams(
            collective_id=0, has_side_effects=True, vmem_limit_bytes=VMEM_COLUMN
        ),
        cost_estimate=pl.CostEstimate(flops=2_000_000_000, bytes_accessed=20_000_000, transcendentals=0),
    )(*[pltpu.with_memory_space_constraint(x, pltpu.HBM) for x in operands + [left]])


def finish_kernel(early, facets, right_ref, cos_ref, sin_ref, near_ref, fwd_ref, done_ref, out_ref, held, ready, done_sem, ready_sem):
    layers, band, grid_size = cos_ref.shape
    slots = out_ref.shape[0]
    half = band // HALVES
    if early:
        sequence = arrivals(facets, lax.axis_index("facet"))
    else:
        sequence = list(range(slots))
    moved = []
    for k in range(early):
        moved.append(pltpu.make_async_copy(done_ref.at[k], out_ref.at[sequence[k]], done_sem.at[k]))
        moved[-1].start()

    def ship(slot, step):
        layer = lax.rem(step, layers)
        rows = pl.ds(pl.multiple_of(lax.div(step, layers) * half, half), half)
        return pltpu.make_async_copy(
            ready.at[layer, rows], out_ref.at[slot, layer, rows], ready_sem.at[step]
        )

    for k in range(early, slots):

        def run(step, carry, k=k):
            if k > early:
                ship(sequence[k - 1], step).wait()
            unit(step, right_ref, sequence[k], near_ref, fwd_ref, cos_ref, sin_ref, held, ready)
            ship(sequence[k], step).start()
            return carry

        lax.fori_loop(0, layers * HALVES, run, 0, unroll=True)
    for step in range(layers * HALVES):
        ship(sequence[slots - 1], step).wait()
    for copy in moved:
        copy.wait()


def finish(right, cos, sin, near, fwd, done, early, facets):
    layers, band, grid_size = cos.shape
    slots = right.shape[0]
    vmem = pl.BlockSpec(memory_space=pltpu.VMEM)
    return pl.pallas_call(
        functools.partial(finish_kernel, early, facets),
        out_shape=jax.ShapeDtypeStruct((slots, layers, band, 2, grid_size), jnp.bfloat16),
        in_specs=[vmem] * 6,
        out_specs=pl.BlockSpec(memory_space=pl.ANY),
        scratch_shapes=[
            pltpu.VMEM((2 * band // HALVES, grid_size), jnp.bfloat16),
            pltpu.VMEM((layers, band, 2, grid_size), jnp.bfloat16),
            pltpu.SemaphoreType.DMA((max(early, 1),)),
            pltpu.SemaphoreType.DMA((layers * HALVES,)),
        ],
        compiler_params=pltpu.CompilerParams(vmem_limit_bytes=VMEM_FINISH),
        cost_estimate=pl.CostEstimate(flops=2_000_000_000, bytes_accessed=20_000_000, transcendentals=0),
    )(right, cos, sin, near, fwd, done)


def local(
    facet_data,
    window,
    screen_phase,
    facet_shift,
    sub_offset,
    win_start,
    win_extent,
    owner_slot,
    layer_w,
):
    facets = lax.axis_size("facet")
    owners = lax.axis_size("sub")
    teams = lax.axis_size("wa")
    strip_rows = facet_data.shape[1]
    facet_len = facet_data.shape[3]
    band, grid_size = screen_phase.shape
    total_subs = owner_slot.shape[0]
    slots = total_subs // owners
    group = facets // slots
    chunk = strip_rows // group
    strip_total = strip_rows * owners * teams
    layers = layer_w.shape[0] // teams
    dims = (facets, owners, teams, strip_rows, facet_len, grid_size, slots, total_subs)

    outer_len = facet_len // LANES
    sig = facet_data[0].reshape(strip_rows, 2, outer_len, LANES).transpose(0, 2, 1, 3)
    shade = window.reshape(outer_len, LANES)
    tables = strip_tables(facet_len, grid_size)
    scalars = (facet_shift, sub_offset, win_start, win_extent, owner_slot, layer_w)
    g_ids, t_ids, c_ids, o_ids, r_ids = np.meshgrid(
        np.arange(group), np.arange(teams), np.arange(2), np.arange(owners), np.arange(chunk), indexing="ij"
    )
    global_row = ((o_ids * teams + t_ids) * strip_rows + g_ids * chunk + r_ids).reshape(1, 1, -1)
    is_imag = c_ids.reshape(1, 1, -1)
    my_rows = np.arange(grid_size).reshape(facets * HALVES, band // HALVES, 1)
    all_cos, all_sin = table(my_rows * global_row, grid_size, -1.0)
    real_rows = np.where(is_imag == 1, -all_sin, all_cos)
    imag_rows = np.where(is_imag == 1, all_cos, all_sin)
    left = np.concatenate([real_rows, imag_rows], 1).astype(jnp.bfloat16)
    left = jnp.asarray(left.reshape(facets, HALVES, 2 * band // HALVES, 2 * strip_total))

    early = facets - 1 if group == 1 and layers * HALVES == PARTS else 0
    right, cos, sin, near, fwd, done = column(scalars, sig, shade, tables, left, screen_phase, dims, layers, early)
    if not early:
        right = right.reshape(slots, 2 * strip_total, grid_size)
    return finish(right, cos, sin, near, fwd, done, early, facets)


def solution(mesh):
    in_specs = (
        P("facet", ("sub", "wa"), None, None),
        P(),
        P("facet", None),
        P(),
        P(),
        P(),
        P(),
        P(),
        P(),
    )
    out_specs = P("sub", "wa", "facet", None, None)
    return jax.shard_map(local, mesh=mesh, in_specs=in_specs, out_specs=out_specs, check_vma=False)
```
